32 devices in a mesh: pair: 2 (over core), shard: 16 (over z, y, x).
Axes of the slice: x: 2, y: 2, z: 4, core: 2. Of those that a mesh axis runs over, the one named last changes fastest.
Arguments:
- master: float32 [3072, 4096], P('shard', 'pair'), may hold values from -1.5 to 1.5
- gradient: float32 [3072, 4096], P('shard', 'pair'), may hold values from -40 to 40
- first_moment: float32 [3072, 4096], P('shard', 'pair'), may hold values from -4 to 4
- second_moment: float32 [3072, 4096], P('shard', 'pair'), may hold values from 0.02 to 4
- max_norm: float32 [1], replicated, may hold values from 768 to 1536
- step_count: int32 [1], replicated, may hold values from 1 to 1000
Outputs:
- new_master: float32 [3072, 4096], P('shard', 'pair')
- new_first: float32 [3072, 4096], P('shard', 'pair')
- new_second: float32 [3072, 4096], P('shard', 'pair')
- compute_codes: bfloat16 [3072, 4096], P('pair')
- block_scales: bfloat16 [3072, 128], P('pair')
The draws below stay inside these ranges and needn't reach their ends.
All inputs are finite; a program needn't handle non-finite values.
Results may differ from the reference program's by a relative error of at most 0.001.
The reference program's roundings to bfloat16 on the way count: a program that leaves them out, or rounds other values in their place, can miss the bound.
Values may be sent and summed in bfloat16 or wider, within the bound.
A program may use at most 192 MiB of HBM per device.

```python
import math
import jax
import jax.numpy as jnp
from jax import lax

ROWS = 3072
COLS = 4096
BLOCK = 32


def draw_gradient(key, part):
    key_heads, key_halves, key_rows, key_noise = jax.random.split(key, 4)
    head_count = (ROWS + 127) // 128
    head_index = jnp.arange(ROWS) // 128
    head_log = jax.random.uniform(key_heads, (head_count,), minval=-2.0, maxval=2.0)
    head_scale = jnp.exp(head_log)[head_index][:, None]
    half_sign = jnp.where(jax.random.bernoulli(key_halves), 1.0, -1.0)
    upper_half = jnp.arange(COLS) >= COLS // 2
    half_scale = jnp.exp(0.7 * half_sign * jnp.where(upper_half, -1.0, 1.0))[None, :]
    row_scale = jnp.exp(jax.random.uniform(key_rows, (ROWS, 1), minval=-0.7, maxval=0.7))
    noise_part = jnp.clip(jax.random.normal(key_noise, (ROWS, COLS)), -6.0, 6.0)
    values = head_scale * half_scale * row_scale * noise_part
    return jnp.clip(values, -40.0, 40.0).astype(jnp.float32)


def block_scale(key, dims, cuts, low, high):
    def one(axis_at, parts):
        heights = jax.random.uniform(jax.random.fold_in(jax.random.fold_in(key, 6), axis_at), (parts,), jnp.float32, low / len(cuts), high / len(cuts))
        return jnp.repeat(jnp.exp(heights), dims[axis_at] // parts).reshape((-1,) + (1,) * (len(dims) - axis_at - 1))

    gain = one(*cuts[0])
    for cut in cuts[1:]:
        gain = gain * one(*cut)
    return gain


def noise(rng, extent, scale, limit, pieces=(), kind=jnp.bfloat16):
    loudness = block_scale(rng, extent, pieces, -0.22, 0.18) if pieces else 1.0
    drawn = jax.random.normal(rng, extent, jnp.float32) * scale * loudness
    return jnp.minimum(jnp.maximum(drawn, -limit), limit).astype(kind)


def setup_inputs(seed: int = 0) -> dict:
    streams_of = jax.random.split(jax.random.key(seed), 7)
    return {
        "master": noise(streams_of[0], (ROWS, COLS), 0.25, 1.5, ((0, 16), (1, 2)), jnp.float32),
        "gradient": draw_gradient(jax.random.fold_in(streams_of[6], 71), 0),
        "first_moment": noise(streams_of[2], (ROWS, COLS), 0.5, 4.0, ((0, 16), (1, 2)), jnp.float32),
        "second_moment": jnp.clip(jnp.exp(math.log(4.0) - 5.2983174 * jax.random.uniform(streams_of[3], (ROWS, COLS), jnp.float32) ** block_scale(streams_of[3], (ROWS, COLS), ((0, 16), (1, 2)), -0.2, 0.2)), 0.02, 4.0),
        "max_norm": jnp.clip(jax.random.uniform(streams_of[4], (1,), jnp.float32, 768.0, 1536.0), 768.0, 1536.0),
        "step_count": jax.random.randint(streams_of[5], (1,), 1, 1001).astype(jnp.int32),
    }


beta_first = 0.9
beta_second = 0.99
learn_rate = 0.01
decay_rate = 0.1
adam_eps = 1e-06
scale_floor = 0.25

def quantize(weights):
    height, width = weights.shape
    blocked = weights.reshape(height, width // BLOCK, BLOCK)
    largest = lax.optimization_barrier(jnp.max(jnp.abs(blocked), axis=2))
    scales = jnp.maximum(largest, scale_floor).astype(jnp.bfloat16)
    divided = blocked / scales.astype(jnp.float32)[:, :, None]
    return (divided.astype(jnp.bfloat16).reshape(height, width), scales)

def adam_update(master, gradient, first_moment, second_moment, max_norm, step_count, squares):
    norm_limit = max_norm[0]
    clip_factor = norm_limit / jnp.maximum(jnp.sqrt(squares), norm_limit)
    clipped = clip_factor * gradient
    new_first = beta_first * first_moment + (1.0 - beta_first) * clipped
    new_second = beta_second * second_moment + (1.0 - beta_second) * clipped * clipped
    counted = step_count[0].astype(jnp.float32)
    first_fix = 1.0 - jnp.power(jnp.full((), beta_first, jnp.float32), counted)
    second_fix = 1.0 - jnp.power(jnp.full((), beta_second, jnp.float32), counted)
    update = new_first / first_fix / (jnp.sqrt(new_second / second_fix) + adam_eps) + decay_rate * master
    new_master = master - learn_rate * update
    return (new_master, new_first, new_second)

def reference(master, gradient, first_moment, second_moment, max_norm, step_count):
    squares = jnp.sum(gradient * gradient)
    new_master, new_first, new_second = adam_update(master, gradient, first_moment, second_moment, max_norm, step_count, squares)
    compute_codes, block_scales = quantize(new_master)
    return (new_master, new_first, new_second, compute_codes, block_scales)
```

```python
import functools

import jax
import jax.numpy as jnp
from jax import lax
from jax.experimental import pallas as pl
from jax.experimental.pallas import tpu as pltpu
from jax.sharding import PartitionSpec as P

BLOCK = 32
LANES = 128

beta_first = 0.9
beta_second = 0.99
learn_rate = 0.01
decay_rate = 0.1
adam_eps = 1e-06
scale_floor = 0.25

MESH = pl.DeviceIdType.MESH
Z, Y, X = 0, 1, 2
PIECES = (
    ((Z, X, Y), (3, 3)),
    ((Z, Y, X), (3, 3)),
    ((X, Y, Z), (2, 1)),
    ((Z, X, Y), (3, 3)),
    ((Z, Y, X), (3, 4)),
    ((Y, X, Z), (2, 2)),
)
SCALE_ORDER = (Z, X, Y)


def grid_of(mesh):
    count = mesh.shape["shard"]
    at = [d.coords for d in mesh.devices.reshape(mesh.shape["pair"], count)[0]]
    sizes = tuple(len({c[d] for c in at}) for d in (2, 1, 0))
    return sizes


def power(base, exponent):
    result = jnp.float32(1.0)
    for bit in range(31):
        factor = jnp.float32(base ** (2**bit))
        result = jnp.where((exponent >> bit) & 1 == 1, result * factor, result)
    return result


def kernel(
    grid, limit_ref, step_ref, master_hbm, gradient_hbm, first_hbm, second_hbm,
    new_master, new_first, new_second, codes, scales,
    master, gradient, first, second, mine, my_scales, wide_scales, their_scales,
    plane_sums, line_sums,
    load_sem, sum_send, plane_recv, line_recv, send_sem, peer_scale_recv, recv_sem, local_sem,
):
    sizes = grid
    depth, high, wide = sizes
    plane = high * wide
    half_depth = depth // 2
    sources = half_depth * plane
    height, width = mine.shape
    tiles = width // LANES
    pieces = len(PIECES)
    core = lax.axis_index("pair")
    chip = lax.axis_index("shard")
    here = (chip // plane, (chip // wide) % high, chip % wide)
    keeper = here[Z] // half_depth
    peer = 1 - core

    def chip_at(at):
        return (at[Z] * high + at[Y]) * wide + at[X]

    def wait_bytes(ref, sem):
        pltpu.make_async_copy(ref, ref, sem).wait()

    loads = [
        pltpu.make_async_copy(source, held, load_sem.at[i])
        for i, (source, held) in enumerate(
            ((gradient_hbm, gradient), (master_hbm, master), (first_hbm, first), (second_hbm, second))
        )
    ]
    loads[0].start()

    barrier = pltpu.get_barrier_semaphore()
    group = 2 * plane
    my_place = core * plane + here[Y] * wide + here[X]

    def greet(device):
        pl.semaphore_signal(barrier, inc=1, device_id=device, device_id_type=MESH)

    for other in range(depth):
        @pl.when(other != here[Z])
        def _():
            for side in range(2):
                greet((side, chip_at((other, here[Y], here[X]))))

    for place in range(group):
        @pl.when(place != my_place)
        def _():
            greet((place // plane, here[Z] * plane + place % plane))

    for load in loads[1:]:
        load.start()
    loads[0].wait()

    def square(i, totals):
        rows = gradient[pl.ds(pl.multiple_of(i * 8, 8), 8), :]
        totals = list(totals)
        for j in range(tiles):
            part = rows[:, j * LANES : (j + 1) * LANES]
            totals[j % 4] = totals[j % 4] + part * part
        return tuple(totals)

    totals = lax.fori_loop(
        0, height // 8, square, tuple(jnp.zeros((8, LANES), jnp.float32) for _ in range(4))
    )
    total = (totals[0] + totals[1]) + (totals[2] + totals[3])
    total = jnp.sum(total, axis=0, keepdims=True)

    pl.semaphore_wait(barrier, group - 1 + 2 * (depth - 1))

    def exchange(value, buffer, place, count, device_of, recv):
        buffer[place] = value

        def copy(other):
            return pltpu.make_async_remote_copy(
                src_ref=buffer.at[place], dst_ref=buffer.at[place],
                send_sem=sum_send, recv_sem=recv,
                device_id=device_of(other), device_id_type=MESH,
            )

        for other in range(count):
            @pl.when(other != place)
            def _():
                copy(other).start()

        others = buffer.at[pl.ds(0, count - 1)]
        wait_bytes(others, recv)
        wait_bytes(others, sum_send)
        return jnp.sum(buffer[...], axis=0)

    total = exchange(
        total, plane_sums, my_place, group,
        lambda place: (place // plane, here[Z] * plane + place % plane), plane_recv,
    )
    total = exchange(
        total, line_sums, here[Z], depth,
        lambda other: (core, chip_at((other, here[Y], here[X]))), line_recv,
    )
    squares = jnp.sum(total, axis=1, keepdims=True)
    norm_limit = jnp.full((1, 1), limit_ref[0], jnp.float32)
    clip_factor = norm_limit / jnp.maximum(jnp.sqrt(squares), norm_limit)
    one = jnp.ones((1, 1), jnp.float32)
    first_gain = one / (one - power(beta_first, step_ref[0]))
    second_gain = one / (one - power(beta_second, step_ref[0]))
    clip_first = ((1.0 - beta_first) * clip_factor)[0, 0]
    clip_second = ((1.0 - beta_second) * clip_factor * clip_factor)[0, 0]
    step_gain = (learn_rate * first_gain)[0, 0]
    second_gain = second_gain[0, 0]
    for load in loads[1:]:
        load.wait()

    def children(source, order):
        last = jnp.int32(-1)
        for i, dim in enumerate(order):
            last = jnp.where(here[dim] != source[dim], i, last)
        ways = []
        for i, dim in enumerate(order):
            if sizes[dim] == 2:
                there = list(here)
                there[dim] = 1 - here[dim]
                ways.append((last < i, chip_at(there)))
            elif sizes[dim] > 2:
                for step in (1, -1):
                    there = list(here)
                    there[dim] = here[dim] + step
                    inside = (there[dim] >= 0) & (there[dim] < sizes[dim])
                    away = (here[dim] - source[dim]) * step > 0
                    ways.append((inside & ((last < i) | ((last == i) & away)), chip_at(there)))
        return ways

    spans = []
    at = [0, 0]
    for _, shares in PIECES:
        sized = [tiles * share // 16 for share in shares]
        spans.append([(at[c], sized[c]) for c in range(2)])
        at = [at[c] + sized[c] for c in range(2)]
    assert at == [tiles, tiles]

    def code_slice(source, column, k):
        row = (chip_at(source) % sources) * height
        start, size = spans[k][column]
        lane = column * width + start * LANES
        return codes.at[pl.ds(pl.multiple_of(row, 16), height), pl.ds(lane, size * LANES)]

    def scale_slice(source):
        row = (chip_at(source) % sources) * height
        return scales.at[pl.ds(pl.multiple_of(row, 16), height), :]

    def tile_block(count):
        return codes.at[pl.ds(0, height), pl.ds(0, count * LANES)]

    my_index = chip % sources

    def own_slice(column, k):
        start, size = spans[k][column]
        return mine.at[:, pl.ds(start * LANES, size * LANES)]

    def own_copy(column, k, to):
        return pltpu.make_async_remote_copy(
            src_ref=own_slice(column, k), dst_ref=code_slice(here, column, k),
            send_sem=send_sem, recv_sem=recv_sem.at[my_index, k],
            device_id=(keeper, to), device_id_type=MESH,
        )

    lane = lax.broadcasted_iota(jnp.int32, (1, LANES), 1)
    spread_row = lax.broadcasted_iota(jnp.int32, (LANES, LANES), 0)
    spread_column = lax.broadcasted_iota(jnp.int32, (LANES, LANES), 1)
    spread = (spread_row == spread_column // BLOCK * BLOCK).astype(jnp.float32).astype(jnp.bfloat16)
    per_tile = LANES // BLOCK
    assert tiles <= BLOCK

    def tile(j, carry):
        where = (slice(None), pl.ds(pl.multiple_of(j * LANES, LANES), LANES))
        weight = master[where]
        slope = gradient[where]
        moment = beta_first * first[where] + clip_first * slope
        power_moment = beta_second * second[where] + clip_second * (slope * slope)
        new_first[where] = moment
        new_second[where] = power_moment
        scaled = power_moment * second_gain
        root = scaled * lax.rsqrt(scaled)
        weight = (1.0 - learn_rate * decay_rate) * weight - step_gain * moment / (root + adam_eps)
        new_master[where] = weight
        largest = jnp.abs(weight)
        shift = BLOCK // 2
        while shift:
            largest = jnp.maximum(largest, pltpu.roll(largest, LANES - shift, axis=1))
            shift //= 2
        scale = jnp.maximum(largest, scale_floor).astype(jnp.bfloat16)
        scale = jnp.dot(scale, spread, preferred_element_type=jnp.float32)
        mine[where] = (weight / scale).astype(jnp.bfloat16)
        wide_scales[...] = jnp.where(lane % BLOCK == j, scale, wide_scales[...])
        return carry

    wide_scales[...] = jnp.zeros_like(wide_scales)
    sent = jnp.int32(0)
    for c in range(2):
        def own_pieces(sent):
            for k, (order, _) in enumerate(PIECES):
                start, size = spans[k][c]
                lax.fori_loop(start, start + size, tile, 0)
                for used, to in children(here, order):
                    @pl.when(used)
                    def _():
                        own_copy(c, k, to).start()

                    sent = sent + jnp.where(used, size, 0)

                @pl.when(c == keeper)
                def _():
                    pltpu.make_async_copy(
                        own_slice(c, k), code_slice(here, c, k), local_sem
                    ).start()

                @pl.when(c != keeper)
                def _():
                    own_copy(c, k, chip).start()

                sent = sent + jnp.where(c != keeper, size, 0)
            return sent

        sent = lax.cond(core == c, own_pieces, lambda s: s, sent)

    place_row = spread_row % BLOCK
    target = (core * tiles + place_row) * per_tile + spread_row // BLOCK
    pick = ((place_row < tiles) & (spread_column == target)).astype(jnp.float32)
    placed = jnp.dot(
        wide_scales[...].astype(jnp.bfloat16), pick.astype(jnp.bfloat16),
        preferred_element_type=jnp.float32,
    )
    my_scales[...] = placed.astype(jnp.bfloat16)
    peer_scales = pltpu.make_async_remote_copy(
        src_ref=my_scales, dst_ref=their_scales, send_sem=send_sem,
        recv_sem=peer_scale_recv, device_id=(peer, chip), device_id_type=MESH,
    )

    def scale_copy(source, to):
        return pltpu.make_async_remote_copy(
            src_ref=scale_slice(source), dst_ref=scale_slice(source),
            send_sem=send_sem, recv_sem=recv_sem.at[chip_at(source) % sources, pieces],
            device_id=(core, to), device_id_type=MESH,
        )

    @pl.when(core != keeper)
    def _():
        peer_scales.start()

    @pl.when(core == keeper)
    def _():
        peer_scales.wait_recv()
        merged = my_scales[...] + their_scales[...]
        row = pl.ds(pl.multiple_of(my_index * height, 16), height)
        scales[row, :] = merged
        for used, to in children(here, SCALE_ORDER):
            @pl.when(used)
            def _():
                scale_copy(here, to).start()

    sent = sent + jnp.where(core != keeper, 1, 0)
    for used, _ in children(here, SCALE_ORDER):
        sent = sent + jnp.where((core == keeper) & used, 1, 0)

    low = core * half_depth
    top = low + half_depth - 1

    def source_of(q):
        i, j = q // plane, q % plane
        inside = low + (here[Z] - low + i + depth) % half_depth
        z = jnp.where(here[Z] >= top, top - i, jnp.where(here[Z] <= low, low + i, inside))
        return (z, (here[Y] + j // wide) % high, (here[X] + j % wide) % wide)

    def code_copy(source, column, k, to):
        part = code_slice(source, column, k)
        return pltpu.make_async_remote_copy(
            src_ref=part, dst_ref=part, send_sem=send_sem,
            recv_sem=recv_sem.at[chip_at(source) % sources, k],
            device_id=(core, to), device_id_type=MESH,
        )

    def item_of(t):
        return t // (pieces + 1), t % (pieces + 1)

    def forward(t, sent):
        q, which = item_of(t)
        source = source_of(q)
        index = chip_at(source) % sources
        mine_too = chip_at(source) == chip

        for k, (order, _) in enumerate(PIECES):
            both = spans[k][0][1] + spans[k][1][1]

            for c in range(2):
                @pl.when((which == k) & mine_too & (core == c))
                def _():
                    wait_bytes(code_slice(source, 1 - c, k), recv_sem.at[index, k])

            for_k = (which == k) & jnp.logical_not(mine_too)
            ways = children(source, order)

            @pl.when(for_k)
            def _():
                wait_bytes(tile_block(both), recv_sem.at[index, k])
                for used, to in ways:
                    @pl.when(used)
                    def _():
                        for column in range(2):
                            code_copy(source, column, k, to).start()

            for used, _ in ways:
                sent = sent + jnp.where(for_k & used, both, 0)

        for_scale = (which == pieces) & jnp.logical_not(mine_too)
        ways = children(source, SCALE_ORDER)

        @pl.when(for_scale)
        def _():
            wait_bytes(scale_slice(source), recv_sem.at[index, pieces])
            for used, to in ways:
                @pl.when(used)
                def _():
                    scale_copy(source, to).start()

        for used, _ in ways:
            sent = sent + jnp.where(for_scale & used, 1, 0)
        return sent

    sent = lax.fori_loop(0, sources * (pieces + 1), forward, sent)

    @pl.when(core == keeper)
    def _():
        wait_bytes(mine, local_sem)

    most = 1
    while 2 * most <= 2 * tiles:
        most *= 2

    def drain(i, carry):
        wait_bytes(tile_block(most), send_sem)
        return carry

    lax.fori_loop(0, sent // most, drain, 0)
    part = most // 2
    while part:
        @pl.when((sent // part) % 2 == 1)
        def _():
            wait_bytes(tile_block(part), send_sem)

        part //= 2


def per_device(grid, master, gradient, first_moment, second_moment, max_norm, step_count):
    height, width = master.shape
    plane = grid[1] * grid[2]
    sources = grid[0] * plane // 2
    pieces = len(PIECES)
    kept = sources * height
    state = jax.ShapeDtypeStruct(master.shape, jnp.float32)
    held = pltpu.VMEM(master.shape, jnp.float32)
    narrow = pltpu.VMEM((height, LANES), jnp.bfloat16)
    dma = pltpu.SemaphoreType.DMA
    vmem = pl.BlockSpec(memory_space=pltpu.VMEM)
    smem = pl.BlockSpec(memory_space=pltpu.SMEM)
    hbm = pl.BlockSpec(memory_space=pltpu.HBM)
    free = pl.BlockSpec(memory_space=pl.ANY)
    state_in = [
        pltpu.with_memory_space_constraint(a, pltpu.HBM)
        for a in (master, gradient, first_moment, second_moment)
    ]
    results = pl.pallas_call(
        functools.partial(kernel, grid),
        out_shape=(
            state, state, state,
            jax.ShapeDtypeStruct((kept, 2 * width), jnp.bfloat16),
            jax.ShapeDtypeStruct((kept, 2 * width // BLOCK), jnp.bfloat16),
        ),
        in_specs=[smem, smem, hbm, hbm, hbm, hbm],
        out_specs=(vmem, vmem, vmem, free, vmem),
        scratch_shapes=[
            held, held, held, held,
            pltpu.VMEM((height, width), jnp.bfloat16),
            narrow,
            pltpu.VMEM((height, LANES), jnp.float32),
            narrow,
            pltpu.VMEM((2 * plane, 1, LANES), jnp.float32),
            pltpu.VMEM((grid[0], 1, LANES), jnp.float32),
            dma((4,)), dma(()), dma(()), dma(()), dma(()), dma(()),
            dma((sources, pieces + 1)), dma(()),
        ],
        compiler_params=pltpu.CompilerParams(
            collective_id=0, has_side_effects=True, vmem_limit_bytes=KERNEL_VMEM
        ),
    )(max_norm, step_count, *state_in)
    return pl.pallas_call(
        flush,
        out_shape=tuple(jax.ShapeDtypeStruct(r.shape, r.dtype) for r in results),
        in_specs=[free] * len(results),
        out_specs=(hbm,) * len(results),
        scratch_shapes=[dma((len(results), PARTS))],
        compiler_params=pltpu.CompilerParams(vmem_limit_bytes=FLUSH_VMEM),
    )(*results)


def flush(*refs):
    count = len(refs) // 2
    sem = refs[-1]
    copies = []
    for i, (held, out) in enumerate(zip(refs[:count], refs[count:-1])):
        rows = held.shape[0] // PARTS
        for part in range(PARTS):
            span = pl.ds(part * rows, rows)
            copies.append(pltpu.make_async_copy(held.at[span], out.at[span], sem.at[i, part]))
    for copy in copies:
        copy.start()
    for copy in copies:
        copy.wait()


PARTS = 2
FLUSH_VMEM = 1024 * 1024


KERNEL_VMEM = 16 * 1024 * 1024


def solution(mesh):
    return jax.shard_map(
        functools.partial(per_device, grid_of(mesh)),
        mesh=mesh,
        in_specs=(
            P("shard", "pair"),
            P("shard", "pair"),
            P("shard", "pair"),
            P("shard", "pair"),
            P(),
            P(),
        ),
        out_specs=(
            P("shard", "pair"),
            P("shard", "pair"),
            P("shard", "pair"),
            P("pair", None),
            P("pair", None),
        ),
        check_vma=False,
    )
```

```python
import functools

import jax
import jax.numpy as jnp
from jax import lax
from jax.experimental import pallas as pl
from jax.experimental.pallas import tpu as pltpu
from jax.sharding import PartitionSpec as P

BLOCK = 32
LANES = 128

beta_first = 0.9
beta_second = 0.99
learn_rate = 0.01
decay_rate = 0.1
adam_eps = 1e-06
scale_floor = 0.25

MESH = pl.DeviceIdType.MESH
Z, Y, X = 0, 1, 2
PIECES = (
    ((Z, X, Y), 0, 4),
    ((Z, Y, X), 1, 4),
    ((Y, X, Z), 0, 4),
    ((X, Y, Z), 1, 3),
    ((Z, Y, X), 0, 4),
    ((Z, X, Y), 1, 4),
    ((Z, X, Y), 0, 4),
    ((Z, Y, X), 1, 5),
)
SCALE_ORDER = (Z, X, Y)
ITEMS = {
    (4, 2, 2): (
        (0, 2), (0, 5), (0, 0), (0, 8), (0, 7), (0, 6), (0, 3), (0, 1), (0, 4), (2, 2),
        (1, 0), (4, 1), (2, 0), (1, 1), (2, 5), (1, 2), (1, 7), (2, 4), (4, 0), (1, 4),
        (4, 6), (4, 2), (1, 8), (1, 6), (2, 1), (2, 7), (1, 3), (3, 3), (5, 0), (6, 0),
        (2, 3), (4, 4), (4, 5), (4, 7), (4, 3), (6, 1), (1, 5), (3, 8), (2, 8), (3, 0),
        (6, 2), (3, 7), (7, 0), (2, 6), (7, 3), (3, 2), (4, 8), (6, 3), (6, 4), (6, 5),
        (3, 1), (5, 1), (5, 5), (5, 2), (5, 4), (5, 6), (6, 7), (3, 6), (7, 2), (6, 8),
        (5, 8), (5, 7), (6, 6), (5, 3), (7, 4), (3, 4), (3, 5), (7, 6), (7, 1), (7, 5),
        (7, 8), (7, 7),
    ),
}
WORD = 4
ONE_STAGE = 32


def grid_of(mesh):
    count = mesh.shape["shard"]
    at = [d.coords for d in mesh.devices.reshape(mesh.shape["pair"], count)[0]]
    sizes = tuple(len({c[d] for c in at}) for d in (2, 1, 0))
    return sizes


def power(base, exponent):
    result = jnp.float32(1.0)
    for bit in range(31):
        factor = jnp.float32(base ** (2**bit))
        result = jnp.where((exponent >> bit) & 1 == 1, result * factor, result)
    return result


def kernel(
    grid, limit_ref, step_ref, master_hbm, gradient_hbm, first_hbm, second_hbm,
    new_master, new_first, new_second, codes, scales,
    master, gradient, first, second, mine, my_scales, wide_scales, their_scales,
    group_sums, line_sums,
    load_sem, sum_send, group_recv, line_recv, send_sem, peer_scale_recv, recv_sem, local_sem,
):
    sizes = grid
    depth, high, wide = sizes
    plane = high * wide
    half_depth = depth // 2
    sources = half_depth * plane
    height, width = mine.shape
    tiles = width // LANES
    pieces = len(PIECES)
    core = lax.axis_index("pair")
    chip = lax.axis_index("shard")
    here = (chip // plane, (chip // wide) % high, chip % wide)
    keeper = here[Z] // half_depth
    peer = 1 - core

    def chip_at(at):
        return (at[Z] * high + at[Y]) * wide + at[X]

    def wait_bytes(ref, sem):
        pltpu.make_async_copy(ref, ref, sem).wait()

    loads = [
        pltpu.make_async_copy(source, held, load_sem.at[i])
        for i, (source, held) in enumerate(
            ((gradient_hbm, gradient), (master_hbm, master), (first_hbm, first), (second_hbm, second))
        )
    ]
    loads[0].start()
    barrier = pltpu.get_barrier_semaphore()
    chips = depth * plane
    one_stage = 2 * chips <= ONE_STAGE
    if one_stage:
        group = 2 * chips
        my_place = core * chips + chip
    else:
        group = 2 * plane
        my_place = core * plane + here[Y] * wide + here[X]

    def member(place):
        if one_stage:
            return (place // chips, place % chips)
        return (place // plane, here[Z] * plane + place % plane)

    def greet(device):
        pl.semaphore_signal(barrier, inc=1, device_id=device, device_id_type=MESH)

    def greet_member(place, carry):
        @pl.when(place != my_place)
        def _():
            greet(member(place))

        return carry

    lax.fori_loop(0, group, greet_member, 0)
    greeted = group - 1
    if not one_stage:
        for other in range(depth):
            @pl.when(other != here[Z])
            def _():
                for side in range(2):
                    greet((side, chip_at((other, here[Y], here[X]))))

        greeted += 2 * (depth - 1)

    for load in loads[1:]:
        load.start()
    loads[0].wait()

    def square(i, totals):
        rows = gradient[pl.ds(pl.multiple_of(i * 8, 8), 8), :]
        totals = list(totals)
        for j in range(tiles):
            part = rows[:, j * LANES : (j + 1) * LANES]
            totals[j % 4] = totals[j % 4] + part * part
        return tuple(totals)

    totals = lax.fori_loop(
        0, height // 8, square, tuple(jnp.zeros((8, LANES), jnp.float32) for _ in range(4))
    )
    total = (totals[0] + totals[1]) + (totals[2] + totals[3])
    total = jnp.sum(total, axis=0, keepdims=True)

    one = jnp.ones((1, 1), jnp.float32)
    first_gain = one / (one - power(beta_first, step_ref[0]))
    second_gain = one / (one - power(beta_second, step_ref[0]))
    step_gain = jnp.broadcast_to(learn_rate * first_gain, (1, LANES))
    second_gain = jnp.broadcast_to(second_gain, (1, LANES))
    norm_limit = jnp.full((1, 1), limit_ref[0], jnp.float32)

    pl.semaphore_wait(barrier, greeted)

    def exchange(value, buffer, place, count, device_of, recv):
        buffer[place] = value

        def copy(other):
            return pltpu.make_async_remote_copy(
                src_ref=buffer.at[place], dst_ref=buffer.at[place],
                send_sem=sum_send, recv_sem=recv,
                device_id=device_of(other), device_id_type=MESH,
            )

        def send(other, carry):
            @pl.when(other != place)
            def _():
                copy(other).start()

            return carry

        lax.fori_loop(0, count, send, 0)
        others = buffer.at[pl.ds(0, count - 1)]
        wait_bytes(others, recv)
        wait_bytes(others, sum_send)
        return jnp.sum(buffer[pl.ds(0, count)], axis=0)

    total = exchange(total, group_sums, my_place, group, member, group_recv)
    if not one_stage:
        total = exchange(
            total, line_sums, here[Z], depth,
            lambda other: (core, chip_at((other, here[Y], here[X]))), line_recv,
        )
    squares = jnp.sum(total, axis=1, keepdims=True)
    clip_factor = norm_limit / jnp.maximum(jnp.sqrt(squares), norm_limit)
    clip_factor = jnp.broadcast_to(clip_factor, (1, LANES))
    clip_first = (1.0 - beta_first) * clip_factor
    clip_second = (1.0 - beta_second) * clip_factor * clip_factor
    for load in loads[1:]:
        load.wait()

    def children(source, order):
        last = jnp.int32(-1)
        for i, dim in enumerate(order):
            last = jnp.where(here[dim] != source[dim], i, last)
        ways = []
        for i, dim in enumerate(order):
            if sizes[dim] == 2:
                there = list(here)
                there[dim] = 1 - here[dim]
                ways.append((last < i, chip_at(there)))
            elif sizes[dim] > 2:
                for step in (1, -1):
                    there = list(here)
                    there[dim] = here[dim] + step
                    inside = (there[dim] >= 0) & (there[dim] < sizes[dim])
                    away = (here[dim] - source[dim]) * step > 0
                    ways.append((inside & ((last < i) | ((last == i) & away)), chip_at(there)))
        return ways

    spans = []
    at = [0, 0]
    for _, column, share in PIECES:
        spans.append((at[column], tiles * share // 16))
        at[column] += spans[-1][1]
    assert at == [tiles, tiles]

    def code_part(source, column, start, size):
        row = (chip_at(source) % sources) * height
        lane = column * width + start * LANES
        return codes.at[pl.ds(pl.multiple_of(row, 16), height), pl.ds(lane, size * LANES)]

    def code_slice(source, k):
        return code_part(source, PIECES[k][1], *spans[k])

    def scale_slice(source):
        row = (chip_at(source) % sources) * height
        return scales.at[pl.ds(pl.multiple_of(row, 16), height), :]

    def tile_block(count):
        return codes.at[pl.ds(0, height), pl.ds(0, count * LANES)]

    my_index = chip % sources

    def own_slice(start, size):
        return mine.at[:, pl.ds(start * LANES, size * LANES)]

    def own_copy(column, k, start, size, to):
        return pltpu.make_async_remote_copy(
            src_ref=own_slice(start, size), dst_ref=code_part(here, column, start, size),
            send_sem=send_sem, recv_sem=recv_sem.at[my_index, k],
            device_id=(keeper, to), device_id_type=MESH,
        )

    lane = lax.broadcasted_iota(jnp.int32, (1, LANES), 1)
    spread_row = lax.broadcasted_iota(jnp.int32, (LANES, LANES), 0)
    spread_column = lax.broadcasted_iota(jnp.int32, (LANES, LANES), 1)
    spread = (spread_row == spread_column // BLOCK * BLOCK).astype(jnp.float32).astype(jnp.bfloat16)
    per_tile = LANES // BLOCK
    assert tiles <= BLOCK

    def tile(j, carry):
        where = (slice(None), pl.ds(pl.multiple_of(j * LANES, LANES), LANES))
        weight = master[where]
        slope = gradient[where]
        moment = beta_first * first[where] + clip_first * slope
        power_moment = beta_second * second[where] + clip_second * (slope * slope)
        new_first[where] = moment
        new_second[where] = power_moment
        scaled = power_moment * second_gain
        root = scaled * lax.rsqrt(scaled)
        weight = (1.0 - learn_rate * decay_rate) * weight - step_gain * moment / (root + adam_eps)
        new_master[where] = weight
        largest = jnp.abs(weight)
        shift = BLOCK // 2
        while shift:
            largest = jnp.maximum(largest, pltpu.roll(largest, LANES - shift, axis=1))
            shift //= 2
        scale = jnp.maximum(largest, scale_floor).astype(jnp.bfloat16)
        scale = jnp.dot(scale, spread, preferred_element_type=jnp.float32)
        mine[where] = (weight / scale).astype(jnp.bfloat16)
        wide_scales[...] = jnp.where(lane % BLOCK == j, scale, wide_scales[...])
        return carry

    wide_scales[...] = jnp.zeros_like(wide_scales)
    sent = jnp.int32(0)
    for c in range(2):
        def own_pieces(sent):
            for k, (order, column, _) in enumerate(PIECES):
                if column != c:
                    continue
                start, size = spans[k]
                parts = ((0, 1), (1, size - 1)) if start == 0 and size > 1 else ((0, size),)
                for offset, part in parts:
                    begin = start + offset
                    lax.fori_loop(begin, begin + part, tile, 0)
                    for used, to in children(here, order):
                        @pl.when(used)
                        def _():
                            own_copy(c, k, begin, part, to).start()

                        sent = sent + jnp.where(used, part, 0)

                    @pl.when(c == keeper)
                    def _():
                        pltpu.make_async_copy(
                            own_slice(begin, part), code_part(here, c, begin, part), local_sem
                        ).start()

                    @pl.when(c != keeper)
                    def _():
                        own_copy(c, k, begin, part, chip).start()

                    sent = sent + jnp.where(c != keeper, part, 0)
            return sent

        sent = lax.cond(core == c, own_pieces, lambda s: s, sent)

    place_row = spread_row % BLOCK
    target = (core * tiles + place_row) * per_tile + spread_row // BLOCK
    pick = ((place_row < tiles) & (spread_column == target)).astype(jnp.float32)
    placed = jnp.dot(
        wide_scales[...].astype(jnp.bfloat16), pick.astype(jnp.bfloat16),
        preferred_element_type=jnp.float32,
    )
    my_scales[...] = placed.astype(jnp.bfloat16)
    peer_scales = pltpu.make_async_remote_copy(
        src_ref=my_scales, dst_ref=their_scales, send_sem=send_sem,
        recv_sem=peer_scale_recv, device_id=(peer, chip), device_id_type=MESH,
    )

    def scale_copy(source, to):
        return pltpu.make_async_remote_copy(
            src_ref=scale_slice(source), dst_ref=scale_slice(source),
            send_sem=send_sem, recv_sem=recv_sem.at[chip_at(source) % sources, pieces],
            device_id=(core, to), device_id_type=MESH,
        )

    @pl.when(core != keeper)
    def _():
        peer_scales.start()

    @pl.when(core == keeper)
    def _():
        peer_scales.wait_recv()
        merged = my_scales[...] + their_scales[...]
        row = pl.ds(pl.multiple_of(my_index * height, 16), height)
        scales[row, :] = merged
        for used, to in children(here, SCALE_ORDER):
            @pl.when(used)
            def _():
                scale_copy(here, to).start()

    sent = sent + jnp.where(core != keeper, 1, 0)
    for used, _ in children(here, SCALE_ORDER):
        sent = sent + jnp.where((core == keeper) & used, 1, 0)

    low = core * half_depth
    top = low + half_depth - 1

    def source_of(q):
        i, j = q // plane, q % plane
        inside = low + (here[Z] - low + i + depth) % half_depth
        z = jnp.where(here[Z] >= top, top - i, jnp.where(here[Z] <= low, low + i, inside))
        return (z, (here[Y] + j // wide) % high, (here[X] + j % wide) % wide)

    def code_copy(source, k, to):
        part = code_slice(source, k)
        return pltpu.make_async_remote_copy(
            src_ref=part, dst_ref=part, send_sem=send_sem,
            recv_sem=recv_sem.at[chip_at(source) % sources, k],
            device_id=(core, to), device_id_type=MESH,
        )

    items = ITEMS.get(sizes)
    words = []
    if items:
        assert sorted(items) == [(q, k) for q in range(sources) for k in range(pieces + 1)]
        for start in range(0, len(items), WORD):
            chunk = items[start : start + WORD]
            words.append(sum((16 * q + k) << (7 * i) for i, (q, k) in enumerate(chunk)))

    def item_of(t):
        if not words:
            return t // (pieces + 1), t % (pieces + 1)
        word = jnp.int32(0)
        for i, held in enumerate(words):
            word = jnp.where(t // WORD == i, held, word)
        item = (word >> (7 * (t % WORD))) % 128
        return item // 16, item % 16

    def forward(t, sent):
        q, which = item_of(t)
        source = source_of(q)
        index = chip_at(source) % sources
        mine_too = chip_at(source) == chip

        for k, (order, column, _) in enumerate(PIECES):
            @pl.when((which == k) & jnp.logical_not(mine_too & (core == column)))
            def _():
                wait_bytes(code_slice(source, k), recv_sem.at[index, k])

            for_k = (which == k) & jnp.logical_not(mine_too)
            ways = children(source, order)

            @pl.when(for_k)
            def _():
                for used, to in ways:
                    @pl.when(used)
                    def _():
                        code_copy(source, k, to).start()

            for used, _ in ways:
                sent = sent + jnp.where(for_k & used, spans[k][1], 0)

        for_scale = (which == pieces) & jnp.logical_not(mine_too)
        ways = children(source, SCALE_ORDER)

        @pl.when(for_scale)
        def _():
            wait_bytes(scale_slice(source), recv_sem.at[index, pieces])
            for used, to in ways:
                @pl.when(used)
                def _():
                    scale_copy(source, to).start()

        for used, _ in ways:
            sent = sent + jnp.where(for_scale & used, 1, 0)
        return sent

    sent = lax.fori_loop(0, sources * (pieces + 1), forward, sent)

    @pl.when(core == keeper)
    def _():
        wait_bytes(mine, local_sem)

    most = 1
    while 2 * most <= 2 * tiles:
        most *= 2

    def drain(i, carry):
        wait_bytes(tile_block(most), send_sem)
        return carry

    lax.fori_loop(0, sent // most, drain, 0)
    part = most // 2
    while part:
        @pl.when((sent // part) % 2 == 1)
        def _():
            wait_bytes(tile_block(part), send_sem)

        part //= 2


def per_device(grid, master, gradient, first_moment, second_moment, max_norm, step_count):
    height, width = master.shape
    plane = grid[1] * grid[2]
    sources = grid[0] * plane // 2
    pieces = len(PIECES)
    kept = sources * height
    state = jax.ShapeDtypeStruct(master.shape, jnp.float32)
    held = pltpu.VMEM(master.shape, jnp.float32)
    narrow = pltpu.VMEM((height, LANES), jnp.bfloat16)
    dma = pltpu.SemaphoreType.DMA
    vmem = pl.BlockSpec(memory_space=pltpu.VMEM)
    smem = pl.BlockSpec(memory_space=pltpu.SMEM)
    hbm = pl.BlockSpec(memory_space=pltpu.HBM)
    free = pl.BlockSpec(memory_space=pl.ANY)
    state_in = [
        pltpu.with_memory_space_constraint(a, pltpu.HBM)
        for a in (master, gradient, first_moment, second_moment)
    ]
    results = pl.pallas_call(
        functools.partial(kernel, grid),
        out_shape=(
            state, state, state,
            jax.ShapeDtypeStruct((kept, 2 * width), jnp.bfloat16),
            jax.ShapeDtypeStruct((kept, 2 * width // BLOCK), jnp.bfloat16),
        ),
        in_specs=[smem, smem, hbm, hbm, hbm, hbm],
        out_specs=(vmem, vmem, vmem, free, vmem),
        scratch_shapes=[
            held, held, held, held,
            pltpu.VMEM((height, width), jnp.bfloat16),
            narrow,
            pltpu.VMEM((height, LANES), jnp.float32),
            narrow,
            pltpu.VMEM((max(2 * plane, ONE_STAGE), 1, LANES), jnp.float32),
            pltpu.VMEM((grid[0], 1, LANES), jnp.float32),
            dma((4,)), dma(()), dma(()), dma(()), dma(()), dma(()),
            dma((sources, pieces + 1)), dma(()),
        ],
        compiler_params=pltpu.CompilerParams(
            collective_id=0, has_side_effects=True, vmem_limit_bytes=KERNEL_VMEM
        ),
    )(max_norm, step_count, *state_in)
    return pl.pallas_call(
        flush,
        out_shape=tuple(jax.ShapeDtypeStruct(r.shape, r.dtype) for r in results),
        in_specs=[free] * len(results),
        out_specs=(hbm,) * len(results),
        scratch_shapes=[dma((len(results), PARTS))],
        compiler_params=pltpu.CompilerParams(vmem_limit_bytes=FLUSH_VMEM),
    )(*results)


def flush(*refs):
    count = len(refs) // 2
    sem = refs[-1]
    copies = []
    for i, (held, out) in enumerate(zip(refs[:count], refs[count:-1])):
        rows = held.shape[0] // PARTS
        for part in range(PARTS):
            span = pl.ds(part * rows, rows)
            copies.append(pltpu.make_async_copy(held.at[span], out.at[span], sem.at[i, part]))
    for copy in copies:
        copy.start()
    for copy in copies:
        copy.wait()


PARTS = 2
FLUSH_VMEM = 1024 * 1024


KERNEL_VMEM = 16 * 1024 * 1024


def solution(mesh):
    return jax.shard_map(
        functools.partial(per_device, grid_of(mesh)),
        mesh=mesh,
        in_specs=(
            P("shard", "pair"),
            P("shard", "pair"),
            P("shard", "pair"),
            P("shard", "pair"),
            P(),
            P(),
        ),
        out_specs=(
            P("shard", "pair"),
            P("shard", "pair"),
            P("shard", "pair"),
            P("pair", None),
            P("pair", None),
        ),
        check_vma=False,
    )
```

```python
import functools

import jax
import jax.numpy as jnp
from jax import lax
from jax.experimental import pallas as pl
from jax.experimental.pallas import tpu as pltpu
from jax.sharding import PartitionSpec as P

BLOCK = 32
LANES = 128

beta_first = 0.9
beta_second = 0.99
learn_rate = 0.01
decay_rate = 0.1
adam_eps = 1e-06
scale_floor = 0.25

MESH = pl.DeviceIdType.MESH
Z, Y, X = 0, 1, 2
PIECES = (
    ((Z, X, Y), 0, 4),
    ((Y, X, Z), 1, 2),
    ((Z, Y, X), 0, 4),
    ((Z, Y, X), 1, 4),
    ((X, Y, Z), 0, 5),
    ((Z, X, Y), 1, 6),
    ((Z, X, Y), 0, 3),
    ((Z, Y, X), 1, 4),
)
SCALE_ORDER = (Y, Z, X)
ITEMS = {
    (4, 2, 2): (
        (0, 3), (1, 4), (0, 6), (4, 3), (0, 0), (2, 1), (4, 5), (4, 0), (1, 1), (3, 4),
        (4, 6), (2, 8), (0, 2), (4, 8), (1, 6), (4, 7), (2, 3), (0, 7), (6, 3), (6, 8),
        (6, 0), (5, 0), (6, 5), (2, 6), (0, 8), (2, 0), (2, 2), (4, 1), (3, 8), (3, 1),
        (0, 4), (0, 5), (4, 2), (1, 7), (7, 4), (1, 0), (4, 4), (1, 2), (5, 5), (5, 6),
        (2, 4), (6, 6), (7, 1), (5, 3), (2, 7), (6, 7), (5, 4), (1, 5), (5, 8), (7, 3),
        (6, 2), (1, 8), (6, 4), (3, 6), (1, 3), (5, 1), (0, 1), (2, 5), (3, 3), (7, 0),
        (3, 0), (7, 8), (3, 7), (5, 7), (7, 5), (3, 2), (5, 2), (7, 6), (6, 1), (7, 7),
        (3, 5), (7, 2),
    ),
}
WORD = 4
ONE_STAGE = 32


def grid_of(mesh):
    count = mesh.shape["shard"]
    at = [d.coords for d in mesh.devices.reshape(mesh.shape["pair"], count)[0]]
    sizes = tuple(len({c[d] for c in at}) for d in (2, 1, 0))
    return sizes


def power(base, exponent):
    result = jnp.float32(1.0)
    for bit in range(31):
        factor = jnp.float32(base ** (2**bit))
        result = jnp.where((exponent >> bit) & 1 == 1, result * factor, result)
    return result


def kernel(
    grid, limit_ref, step_ref, master_hbm, gradient_hbm, first_hbm, second_hbm,
    new_master, new_first, new_second, codes, scales,
    master, gradient, first, second, mine, my_scales, wide_scales, their_scales,
    group_sums, line_sums,
    load_sem, sum_send, group_recv, line_recv, send_sem, peer_scale_recv, recv_sem, local_sem,
):
    sizes = grid
    depth, high, wide = sizes
    plane = high * wide
    half_depth = depth // 2
    sources = half_depth * plane
    height, width = mine.shape
    tiles = width // LANES
    pieces = len(PIECES)
    core = lax.axis_index("pair")
    chip = lax.axis_index("shard")
    here = (chip // plane, (chip // wide) % high, chip % wide)
    keeper = here[Z] // half_depth
    peer = 1 - core

    def chip_at(at):
        return (at[Z] * high + at[Y]) * wide + at[X]

    def wait_bytes(ref, sem):
        pltpu.make_async_copy(ref, ref, sem).wait()

    loads = [
        pltpu.make_async_copy(source, held, load_sem.at[i])
        for i, (source, held) in enumerate(
            ((gradient_hbm, gradient), (master_hbm, master), (first_hbm, first), (second_hbm, second))
        )
    ]
    loads[0].start()
    barrier = pltpu.get_barrier_semaphore()
    chips = depth * plane
    one_stage = 2 * chips <= ONE_STAGE
    if one_stage:
        group = 2 * chips
        my_place = core * chips + chip
    else:
        group = 2 * plane
        my_place = core * plane + here[Y] * wide + here[X]

    def member(place):
        if one_stage:
            return (place // chips, place % chips)
        return (place // plane, here[Z] * plane + place % plane)

    def greet(device):
        pl.semaphore_signal(barrier, inc=1, device_id=device, device_id_type=MESH)

    def greet_member(place, carry):
        @pl.when(place != my_place)
        def _():
            greet(member(place))

        return carry

    lax.fori_loop(0, group, greet_member, 0)
    greeted = group - 1
    if not one_stage:
        for other in range(depth):
            @pl.when(other != here[Z])
            def _():
                for side in range(2):
                    greet((side, chip_at((other, here[Y], here[X]))))

        greeted += 2 * (depth - 1)

    for load in loads[1:]:
        load.start()
    loads[0].wait()

    def square(i, totals):
        rows = gradient[pl.ds(pl.multiple_of(i * 8, 8), 8), :]
        totals = list(totals)
        for j in range(tiles):
            part = rows[:, j * LANES : (j + 1) * LANES]
            totals[j % 4] = totals[j % 4] + part * part
        return tuple(totals)

    totals = lax.fori_loop(
        0, height // 8, square, tuple(jnp.zeros((8, LANES), jnp.float32) for _ in range(4))
    )
    total = (totals[0] + totals[1]) + (totals[2] + totals[3])
    total = jnp.sum(total, axis=0, keepdims=True)

    one = jnp.ones((1, 1), jnp.float32)
    first_gain = one / (one - power(beta_first, step_ref[0]))
    second_gain = one / (one - power(beta_second, step_ref[0]))
    step_gain = jnp.broadcast_to(learn_rate * first_gain, (1, LANES))
    second_gain = jnp.broadcast_to(second_gain, (1, LANES))
    norm_limit = jnp.full((1, 1), limit_ref[0], jnp.float32)

    pl.semaphore_wait(barrier, greeted)

    def exchange(value, buffer, place, count, device_of, recv):
        buffer[place] = value

        def copy(other):
            return pltpu.make_async_remote_copy(
                src_ref=buffer.at[place], dst_ref=buffer.at[place],
                send_sem=sum_send, recv_sem=recv,
                device_id=device_of(other), device_id_type=MESH,
            )

        def send(other, carry):
            @pl.when(other != place)
            def _():
                copy(other).start()

            return carry

        lax.fori_loop(0, count, send, 0)
        others = buffer.at[pl.ds(0, count - 1)]
        wait_bytes(others, recv)
        wait_bytes(others, sum_send)
        return jnp.sum(buffer[pl.ds(0, count)], axis=0)

    total = exchange(total, group_sums, my_place, group, member, group_recv)
    if not one_stage:
        total = exchange(
            total, line_sums, here[Z], depth,
            lambda other: (core, chip_at((other, here[Y], here[X]))), line_recv,
        )
    squares = jnp.sum(total, axis=1, keepdims=True)
    clip_factor = norm_limit / jnp.maximum(jnp.sqrt(squares), norm_limit)
    clip_factor = jnp.broadcast_to(clip_factor, (1, LANES))
    clip_first = (1.0 - beta_first) * clip_factor
    clip_second = (1.0 - beta_second) * clip_factor * clip_factor
    for load in loads[1:]:
        load.wait()

    def children(source, order):
        last = jnp.int32(-1)
        for i, dim in enumerate(order):
            last = jnp.where(here[dim] != source[dim], i, last)
        ways = []
        for i, dim in enumerate(order):
            if sizes[dim] == 2:
                there = list(here)
                there[dim] = 1 - here[dim]
                ways.append((last < i, chip_at(there)))
            elif sizes[dim] > 2:
                for step in (1, -1):
                    there = list(here)
                    there[dim] = here[dim] + step
                    inside = (there[dim] >= 0) & (there[dim] < sizes[dim])
                    away = (here[dim] - source[dim]) * step > 0
                    ways.append((inside & ((last < i) | ((last == i) & away)), chip_at(there)))
        return ways

    spans = []
    at = [0, 0]
    for _, column, share in PIECES:
        spans.append((at[column], tiles * share // 16))
        at[column] += spans[-1][1]
    assert at == [tiles, tiles]

    def code_part(source, column, start, size):
        row = (chip_at(source) % sources) * height
        lane = column * width + start * LANES
        return codes.at[pl.ds(pl.multiple_of(row, 16), height), pl.ds(lane, size * LANES)]

    def code_slice(source, k):
        return code_part(source, PIECES[k][1], *spans[k])

    def scale_slice(source):
        row = (chip_at(source) % sources) * height
        return scales.at[pl.ds(pl.multiple_of(row, 16), height), :]

    def tile_block(count):
        return codes.at[pl.ds(0, height), pl.ds(0, count * LANES)]

    my_index = chip % sources

    def own_slice(start, size):
        return mine.at[:, pl.ds(start * LANES, size * LANES)]

    def own_copy(column, k, start, size, to):
        return pltpu.make_async_remote_copy(
            src_ref=own_slice(start, size), dst_ref=code_part(here, column, start, size),
            send_sem=send_sem, recv_sem=recv_sem.at[my_index, k],
            device_id=(keeper, to), device_id_type=MESH,
        )

    lane = lax.broadcasted_iota(jnp.int32, (1, LANES), 1)
    spread_row = lax.broadcasted_iota(jnp.int32, (LANES, LANES), 0)
    spread_column = lax.broadcasted_iota(jnp.int32, (LANES, LANES), 1)
    spread = (spread_row == spread_column // BLOCK * BLOCK).astype(jnp.float32).astype(jnp.bfloat16)
    per_tile = LANES // BLOCK
    assert tiles <= BLOCK

    def tile(j, carry):
        where = (slice(None), pl.ds(pl.multiple_of(j * LANES, LANES), LANES))
        weight = master[where]
        slope = gradient[where]
        moment = beta_first * first[where] + clip_first * slope
        power_moment = beta_second * second[where] + clip_second * (slope * slope)
        new_first[where] = moment
        new_second[where] = power_moment
        scaled = power_moment * second_gain
        root = scaled * lax.rsqrt(scaled)
        weight = (1.0 - learn_rate * decay_rate) * weight - step_gain * moment / (root + adam_eps)
        new_master[where] = weight
        largest = jnp.abs(weight)
        shift = BLOCK // 2
        while shift:
            largest = jnp.maximum(largest, pltpu.roll(largest, LANES - shift, axis=1))
            shift //= 2
        scale = jnp.maximum(largest, scale_floor).astype(jnp.bfloat16)
        scale = jnp.dot(scale, spread, preferred_element_type=jnp.float32)
        mine[where] = (weight / scale).astype(jnp.bfloat16)
        wide_scales[...] = jnp.where(lane % BLOCK == j, scale, wide_scales[...])
        return carry

    wide_scales[...] = jnp.zeros_like(wide_scales)
    sent = jnp.int32(0)
    for c in range(2):
        def own_pieces(sent):
            for k, (order, column, _) in enumerate(PIECES):
                if column != c:
                    continue
                start, size = spans[k]
                parts = ((0, 1), (1, size - 1)) if start == 0 and size > 1 else ((0, size),)
                for offset, part in parts:
                    begin = start + offset
                    lax.fori_loop(begin, begin + part, tile, 0)
                    for used, to in children(here, order):
                        @pl.when(used)
                        def _():
                            own_copy(c, k, begin, part, to).start()

                        sent = sent + jnp.where(used, part, 0)

                    @pl.when(c == keeper)
                    def _():
                        pltpu.make_async_copy(
                            own_slice(begin, part), code_part(here, c, begin, part), local_sem
                        ).start()

                    @pl.when(c != keeper)
                    def _():
                        own_copy(c, k, begin, part, chip).start()

                    sent = sent + jnp.where(c != keeper, part, 0)
            return sent

        sent = lax.cond(core == c, own_pieces, lambda s: s, sent)

    place_row = spread_row % BLOCK
    target = (core * tiles + place_row) * per_tile + spread_row // BLOCK
    pick = ((place_row < tiles) & (spread_column == target)).astype(jnp.float32)
    placed = jnp.dot(
        wide_scales[...].astype(jnp.bfloat16), pick.astype(jnp.bfloat16),
        preferred_element_type=jnp.float32,
    )
    my_scales[...] = placed.astype(jnp.bfloat16)
    peer_scales = pltpu.make_async_remote_copy(
        src_ref=my_scales, dst_ref=their_scales, send_sem=send_sem,
        recv_sem=peer_scale_recv, device_id=(peer, chip), device_id_type=MESH,
    )

    def scale_copy(source, to):
        return pltpu.make_async_remote_copy(
            src_ref=scale_slice(source), dst_ref=scale_slice(source),
            send_sem=send_sem, recv_sem=recv_sem.at[chip_at(source) % sources, pieces],
            device_id=(core, to), device_id_type=MESH,
        )

    @pl.when(core != keeper)
    def _():
        peer_scales.start()

    @pl.when(core == keeper)
    def _():
        peer_scales.wait_recv()
        merged = my_scales[...] + their_scales[...]
        row = pl.ds(pl.multiple_of(my_index * height, 16), height)
        scales[row, :] = merged
        for used, to in children(here, SCALE_ORDER):
            @pl.when(used)
            def _():
                scale_copy(here, to).start()

    sent = sent + jnp.where(core != keeper, 1, 0)
    for used, _ in children(here, SCALE_ORDER):
        sent = sent + jnp.where((core == keeper) & used, 1, 0)

    low = core * half_depth
    top = low + half_depth - 1

    def source_of(q):
        i, j = q // plane, q % plane
        inside = low + (here[Z] - low + i + depth) % half_depth
        z = jnp.where(here[Z] >= top, top - i, jnp.where(here[Z] <= low, low + i, inside))
        return (z, (here[Y] + j // wide) % high, (here[X] + j % wide) % wide)

    def code_copy(source, k, to):
        part = code_slice(source, k)
        return pltpu.make_async_remote_copy(
            src_ref=part, dst_ref=part, send_sem=send_sem,
            recv_sem=recv_sem.at[chip_at(source) % sources, k],
            device_id=(core, to), device_id_type=MESH,
        )

    items = ITEMS.get(sizes)
    words = []
    if items:
        assert sorted(items) == [(q, k) for q in range(sources) for k in range(pieces + 1)]
        for start in range(0, len(items), WORD):
            chunk = items[start : start + WORD]
            words.append(sum((16 * q + k) << (7 * i) for i, (q, k) in enumerate(chunk)))

    def item_of(t):
        if not words:
            return t // (pieces + 1), t % (pieces + 1)
        word = jnp.int32(0)
        for i, held in enumerate(words):
            word = jnp.where(t // WORD == i, held, word)
        item = (word >> (7 * (t % WORD))) % 128
        return item // 16, item % 16

    def forward(t, sent):
        q, which = item_of(t)
        source = source_of(q)
        index = chip_at(source) % sources
        mine_too = chip_at(source) == chip

        for k, (order, column, _) in enumerate(PIECES):
            @pl.when((which == k) & jnp.logical_not(mine_too & (core == column)))
            def _():
                wait_bytes(code_slice(source, k), recv_sem.at[index, k])

            for_k = (which == k) & jnp.logical_not(mine_too)
            ways = children(source, order)

            @pl.when(for_k)
            def _():
                for used, to in ways:
                    @pl.when(used)
                    def _():
                        code_copy(source, k, to).start()

            for used, _ in ways:
                sent = sent + jnp.where(for_k & used, spans[k][1], 0)

        for_scale = (which == pieces) & jnp.logical_not(mine_too)
        ways = children(source, SCALE_ORDER)

        @pl.when(for_scale)
        def _():
            wait_bytes(scale_slice(source), recv_sem.at[index, pieces])
            for used, to in ways:
                @pl.when(used)
                def _():
                    scale_copy(source, to).start()

        for used, _ in ways:
            sent = sent + jnp.where(for_scale & used, 1, 0)
        return sent

    sent = lax.fori_loop(0, sources * (pieces + 1), forward, sent)

    @pl.when(core == keeper)
    def _():
        wait_bytes(mine, local_sem)

    most = 1
    while 2 * most <= 2 * tiles:
        most *= 2

    def drain(i, carry):
        wait_bytes(tile_block(most), send_sem)
        return carry

    lax.fori_loop(0, sent // most, drain, 0)
    part = most // 2
    while part:
        @pl.when((sent // part) % 2 == 1)
        def _():
            wait_bytes(tile_block(part), send_sem)

        part //= 2


def per_device(grid, master, gradient, first_moment, second_moment, max_norm, step_count):
    height, width = master.shape
    plane = grid[1] * grid[2]
    sources = grid[0] * plane // 2
    pieces = len(PIECES)
    kept = sources * height
    state = jax.ShapeDtypeStruct(master.shape, jnp.float32)
    held = pltpu.VMEM(master.shape, jnp.float32)
    narrow = pltpu.VMEM((height, LANES), jnp.bfloat16)
    dma = pltpu.SemaphoreType.DMA
    vmem = pl.BlockSpec(memory_space=pltpu.VMEM)
    smem = pl.BlockSpec(memory_space=pltpu.SMEM)
    hbm = pl.BlockSpec(memory_space=pltpu.HBM)
    free = pl.BlockSpec(memory_space=pl.ANY)
    state_in = [
        pltpu.with_memory_space_constraint(a, pltpu.HBM)
        for a in (master, gradient, first_moment, second_moment)
    ]
    results = pl.pallas_call(
        functools.partial(kernel, grid),
        out_shape=(
            state, state, state,
            jax.ShapeDtypeStruct((kept, 2 * width), jnp.bfloat16),
            jax.ShapeDtypeStruct((kept, 2 * width // BLOCK), jnp.bfloat16),
        ),
        in_specs=[smem, smem, hbm, hbm, hbm, hbm],
        out_specs=(vmem, vmem, vmem, free, vmem),
        scratch_shapes=[
            held, held, held, held,
            pltpu.VMEM((height, width), jnp.bfloat16),
            narrow,
            pltpu.VMEM((height, LANES), jnp.float32),
            narrow,
            pltpu.VMEM((max(2 * plane, ONE_STAGE), 1, LANES), jnp.float32),
            pltpu.VMEM((grid[0], 1, LANES), jnp.float32),
            dma((4,)), dma(()), dma(()), dma(()), dma(()), dma(()),
            dma((sources, pieces + 1)), dma(()),
        ],
        compiler_params=pltpu.CompilerParams(
            collective_id=0, has_side_effects=True, vmem_limit_bytes=KERNEL_VMEM
        ),
    )(max_norm, step_count, *state_in)
    return pl.pallas_call(
        flush,
        out_shape=tuple(jax.ShapeDtypeStruct(r.shape, r.dtype) for r in results),
        in_specs=[free] * len(results),
        out_specs=(hbm,) * len(results),
        scratch_shapes=[dma((len(results), PARTS))],
        compiler_params=pltpu.CompilerParams(vmem_limit_bytes=FLUSH_VMEM),
    )(*results)


def flush(*refs):
    count = len(refs) // 2
    sem = refs[-1]
    copies = []
    for i, (held, out) in enumerate(zip(refs[:count], refs[count:-1])):
        rows = held.shape[0] // PARTS
        for part in range(PARTS):
            span = pl.ds(part * rows, rows)
            copies.append(pltpu.make_async_copy(held.at[span], out.at[span], sem.at[i, part]))
    for copy in copies:
        copy.start()
    for copy in copies:
        copy.wait()


PARTS = 2
FLUSH_VMEM = 1024 * 1024


KERNEL_VMEM = 16 * 1024 * 1024


def solution(mesh):
    return jax.shard_map(
        functools.partial(per_device, grid_of(mesh)),
        mesh=mesh,
        in_specs=(
            P("shard", "pair"),
            P("shard", "pair"),
            P("shard", "pair"),
            P("shard", "pair"),
            P(),
            P(),
        ),
        out_specs=(
            P("shard", "pair"),
            P("shard", "pair"),
            P("shard", "pair"),
            P("pair", None),
            P("pair", None),
        ),
        check_vma=False,
    )
```

```python
import functools

import jax
import jax.numpy as jnp
from jax import lax
from jax.experimental import pallas as pl
from jax.experimental.pallas import tpu as pltpu
from jax.sharding import PartitionSpec as P

BLOCK = 32
LANES = 128

beta_first = 0.9
beta_second = 0.99
learn_rate = 0.01
decay_rate = 0.1
adam_eps = 1e-06
scale_floor = 0.25

MESH = pl.DeviceIdType.MESH
Z, Y, X = 0, 1, 2
PIECES = (
    ((Z, X, Y), 0, 4),
    ((Y, X, Z), 1, 2),
    ((Z, Y, X), 0, 4),
    ((Z, Y, X), 1, 4),
    ((X, Y, Z), 0, 5),
    ((Z, X, Y), 1, 6),
    ((Z, X, Y), 0, 3),
    ((Z, Y, X), 1, 4),
)
SCALE_ORDER = (Y, Z, X)
ROWS = 16
ITEMS = {
    (4, 2, 2): (
        (0, 3), (1, 4), (0, 6), (4, 3), (0, 0), (2, 1), (4, 5), (4, 0), (1, 1), (3, 4),
        (4, 6), (2, 8), (0, 2), (4, 8), (1, 6), (4, 7), (2, 3), (0, 7), (6, 3), (6, 8),
        (6, 0), (5, 0), (6, 5), (2, 6), (0, 8), (2, 0), (2, 2), (4, 1), (3, 8), (3, 1),
        (0, 4), (0, 5), (4, 2), (1, 7), (7, 4), (1, 0), (4, 4), (1, 2), (5, 5), (5, 6),
        (2, 4), (6, 6), (7, 1), (5, 3), (2, 7), (6, 7), (5, 4), (1, 5), (5, 8), (7, 3),
        (6, 2), (1, 8), (6, 4), (3, 6), (1, 3), (5, 1), (0, 1), (2, 5), (3, 3), (7, 0),
        (3, 0), (7, 8), (3, 7), (5, 7), (7, 5), (3, 2), (5, 2), (7, 6), (6, 1), (7, 7),
        (3, 5), (7, 2),
    ),
}
WORD = 4
ONE_STAGE = 32


def grid_of(mesh):
    count = mesh.shape["shard"]
    at = [d.coords for d in mesh.devices.reshape(mesh.shape["pair"], count)[0]]
    sizes = tuple(len({c[d] for c in at}) for d in (2, 1, 0))
    return sizes


def power(base, exponent):
    result = jnp.float32(1.0)
    for bit in range(31):
        factor = jnp.float32(base ** (2**bit))
        result = jnp.where((exponent >> bit) & 1 == 1, result * factor, result)
    return result


def kernel(
    grid, limit_ref, step_ref, master_hbm, gradient_hbm, first_hbm, second_hbm,
    new_master, new_first, new_second, codes, scales,
    master, gradient, first, second, mine, my_scales, wide_scales, their_scales,
    group_sums, line_sums,
    load_sem, sum_send, group_recv, line_recv, send_sem, peer_scale_recv, recv_sem, local_sem,
):
    sizes = grid
    depth, high, wide = sizes
    plane = high * wide
    half_depth = depth // 2
    sources = half_depth * plane
    height, width = mine.shape
    tiles = width // LANES
    pieces = len(PIECES)
    core = lax.axis_index("pair")
    chip = lax.axis_index("shard")
    here = (chip // plane, (chip // wide) % high, chip % wide)
    keeper = here[Z] // half_depth
    peer = 1 - core

    def chip_at(at):
        return (at[Z] * high + at[Y]) * wide + at[X]

    def wait_bytes(ref, sem):
        pltpu.make_async_copy(ref, ref, sem).wait()

    loads = [
        pltpu.make_async_copy(source, held, load_sem.at[i])
        for i, (source, held) in enumerate(
            ((gradient_hbm, gradient), (master_hbm, master), (first_hbm, first), (second_hbm, second))
        )
    ]
    loads[0].start()
    barrier = pltpu.get_barrier_semaphore()
    chips = depth * plane
    one_stage = 2 * chips <= ONE_STAGE
    if one_stage:
        group = 2 * chips
        my_place = core * chips + chip
    else:
        group = 2 * plane
        my_place = core * plane + here[Y] * wide + here[X]

    def member(place):
        if one_stage:
            return (place // chips, place % chips)
        return (place // plane, here[Z] * plane + place % plane)

    def greet(device):
        pl.semaphore_signal(barrier, inc=1, device_id=device, device_id_type=MESH)

    def greet_member(place, carry):
        @pl.when(place != my_place)
        def _():
            greet(member(place))

        return carry

    lax.fori_loop(0, group, greet_member, 0)
    greeted = group - 1
    if not one_stage:
        for other in range(depth):
            @pl.when(other != here[Z])
            def _():
                for side in range(2):
                    greet((side, chip_at((other, here[Y], here[X]))))

        greeted += 2 * (depth - 1)

    for load in loads[1:]:
        load.start()
    loads[0].wait()

    def square(i, totals):
        rows = gradient[pl.ds(pl.multiple_of(i * 8, 8), 8), :]
        totals = list(totals)
        for j in range(tiles):
            part = rows[:, j * LANES : (j + 1) * LANES]
            totals[j % 4] = totals[j % 4] + part * part
        return tuple(totals)

    totals = lax.fori_loop(
        0, height // 8, square, tuple(jnp.zeros((8, LANES), jnp.float32) for _ in range(4))
    )
    total = (totals[0] + totals[1]) + (totals[2] + totals[3])
    total = jnp.sum(total, axis=0, keepdims=True)

    one = jnp.ones((1, 1), jnp.float32)
    first_gain = one / (one - power(beta_first, step_ref[0]))
    second_gain = one / (one - power(beta_second, step_ref[0]))
    step_gain = jnp.broadcast_to(learn_rate * first_gain, (1, LANES))
    second_gain = jnp.broadcast_to(second_gain, (1, LANES))
    norm_limit = jnp.full((1, 1), limit_ref[0], jnp.float32)

    pl.semaphore_wait(barrier, greeted)

    def exchange(value, buffer, place, count, device_of, recv):
        buffer[place] = value

        def copy(other):
            return pltpu.make_async_remote_copy(
                src_ref=buffer.at[place], dst_ref=buffer.at[place],
                send_sem=sum_send, recv_sem=recv,
                device_id=device_of(other), device_id_type=MESH,
            )

        def send(other, carry):
            @pl.when(other != place)
            def _():
                copy(other).start()

            return carry

        lax.fori_loop(0, count, send, 0)
        others = buffer.at[pl.ds(0, count - 1)]
        wait_bytes(others, recv)
        wait_bytes(others, sum_send)
        return jnp.sum(buffer[pl.ds(0, count)], axis=0)

    total = exchange(total, group_sums, my_place, group, member, group_recv)
    if not one_stage:
        total = exchange(
            total, line_sums, here[Z], depth,
            lambda other: (core, chip_at((other, here[Y], here[X]))), line_recv,
        )
    squares = jnp.sum(total, axis=1, keepdims=True)
    clip_factor = norm_limit / jnp.maximum(jnp.sqrt(squares), norm_limit)
    clip_factor = jnp.broadcast_to(clip_factor, (1, LANES))
    clip_first = (1.0 - beta_first) * clip_factor
    clip_second = (1.0 - beta_second) * clip_factor * clip_factor
    for load in loads[1:]:
        load.wait()

    def children(source, order):
        last = jnp.int32(-1)
        for i, dim in enumerate(order):
            last = jnp.where(here[dim] != source[dim], i, last)
        ways = []
        for i, dim in enumerate(order):
            if sizes[dim] == 2:
                there = list(here)
                there[dim] = 1 - here[dim]
                ways.append((last < i, chip_at(there)))
            elif sizes[dim] > 2:
                for step in (1, -1):
                    there = list(here)
                    there[dim] = here[dim] + step
                    inside = (there[dim] >= 0) & (there[dim] < sizes[dim])
                    away = (here[dim] - source[dim]) * step > 0
                    ways.append((inside & ((last < i) | ((last == i) & away)), chip_at(there)))
        return ways

    spans = []
    at = [0, 0]
    for _, column, share in PIECES:
        spans.append((at[column], tiles * share // 16))
        at[column] += spans[-1][1]
    assert at == [tiles, tiles]

    def code_part(source, column, start, size, top_row=0, rows=height):
        row = (chip_at(source) % sources) * height + top_row
        lane = column * width + start * LANES
        return codes.at[pl.ds(pl.multiple_of(row, ROWS), rows), pl.ds(lane, size * LANES)]

    def code_slice(source, k):
        return code_part(source, PIECES[k][1], *spans[k])

    def scale_slice(source):
        row = (chip_at(source) % sources) * height
        return scales.at[pl.ds(pl.multiple_of(row, 16), height), :]

    strips = height // ROWS
    broad = 1
    while 2 * broad <= 2 * tiles:
        broad *= 2

    def blocks(count):
        if count <= broad:
            return codes.at[pl.ds(0, ROWS), pl.ds(0, count * LANES)]
        return codes.at[pl.ds(0, count // broad * ROWS), pl.ds(0, broad * LANES)]

    my_index = chip % sources

    def own_copy(column, k, start, size, top_row, rows, to):
        return pltpu.make_async_remote_copy(
            src_ref=mine.at[pl.ds(top_row, rows), pl.ds(start * LANES, size * LANES)],
            dst_ref=code_part(here, column, start, size, top_row, rows),
            send_sem=send_sem, recv_sem=recv_sem.at[my_index, k],
            device_id=(keeper, to), device_id_type=MESH,
        )

    lane = lax.broadcasted_iota(jnp.int32, (1, LANES), 1)
    spread_row = lax.broadcasted_iota(jnp.int32, (LANES, LANES), 0)
    spread_column = lax.broadcasted_iota(jnp.int32, (LANES, LANES), 1)
    spread = (spread_row == spread_column // BLOCK * BLOCK).astype(jnp.float32).astype(jnp.bfloat16)
    per_tile = LANES // BLOCK
    assert tiles <= BLOCK

    def tile(j, top_row=0, rows=height):
        band = pl.ds(top_row, rows)
        where = (band, pl.ds(pl.multiple_of(j * LANES, LANES), LANES))
        weight = master[where]
        slope = gradient[where]
        moment = beta_first * first[where] + clip_first * slope
        power_moment = beta_second * second[where] + clip_second * (slope * slope)
        new_first[where] = moment
        new_second[where] = power_moment
        scaled = power_moment * second_gain
        root = scaled * lax.rsqrt(scaled)
        weight = (1.0 - learn_rate * decay_rate) * weight - step_gain * moment / (root + adam_eps)
        new_master[where] = weight
        largest = jnp.abs(weight)
        shift = BLOCK // 2
        while shift:
            largest = jnp.maximum(largest, pltpu.roll(largest, LANES - shift, axis=1))
            shift //= 2
        scale = jnp.maximum(largest, scale_floor).astype(jnp.bfloat16)
        scale = jnp.dot(scale, spread, preferred_element_type=jnp.float32)
        mine[where] = (weight / scale).astype(jnp.bfloat16)
        wide_scales[band, :] = jnp.where(lane % BLOCK == j, scale, wide_scales[band, :])

    wide_scales[...] = jnp.zeros_like(wide_scales)
    sent = jnp.int32(0)
    for c in range(2):
        def own_pieces(sent):
            for k, (order, column, _) in enumerate(PIECES):
                if column != c:
                    continue
                start, size = spans[k]
                parts = [(0, size, 0, height)]
                if start == 0:
                    parts = [(i, 1, 0, height) for i in range(size)]
                    cut = strips // 2 * ROWS
                    if cut:
                        parts[:1] = [(0, 1, 0, cut), (0, 1, cut, height - cut)]
                for offset, part, top_row, rows in parts:
                    begin = start + offset

                    def one_tile(j, carry):
                        tile(j, top_row, rows)
                        return carry

                    lax.fori_loop(begin, begin + part, one_tile, 0)
                    amount = part * rows // ROWS
                    for used, to in children(here, order):
                        @pl.when(used)
                        def _():
                            own_copy(c, k, begin, part, top_row, rows, to).start()

                        sent = sent + jnp.where(used, amount, 0)

                    @pl.when(c != keeper)
                    def _():
                        own_copy(c, k, begin, part, top_row, rows, chip).start()

                    sent = sent + jnp.where(c != keeper, amount, 0)
            return sent

        sent = lax.cond(core == c, own_pieces, lambda s: s, sent)

    place_row = spread_row % BLOCK
    target = (core * tiles + place_row) * per_tile + spread_row // BLOCK
    pick = ((place_row < tiles) & (spread_column == target)).astype(jnp.float32)
    placed = jnp.dot(
        wide_scales[...].astype(jnp.bfloat16), pick.astype(jnp.bfloat16),
        preferred_element_type=jnp.float32,
    )
    my_scales[...] = placed.astype(jnp.bfloat16)
    peer_scales = pltpu.make_async_remote_copy(
        src_ref=my_scales, dst_ref=their_scales, send_sem=send_sem,
        recv_sem=peer_scale_recv, device_id=(peer, chip), device_id_type=MESH,
    )

    def scale_copy(source, to):
        return pltpu.make_async_remote_copy(
            src_ref=scale_slice(source), dst_ref=scale_slice(source),
            send_sem=send_sem, recv_sem=recv_sem.at[chip_at(source) % sources, pieces],
            device_id=(core, to), device_id_type=MESH,
        )

    @pl.when(core != keeper)
    def _():
        peer_scales.start()

    @pl.when(core == keeper)
    def _():
        peer_scales.wait_recv()
        merged = my_scales[...] + their_scales[...]
        row = pl.ds(pl.multiple_of(my_index * height, 16), height)
        scales[row, :] = merged
        for used, to in children(here, SCALE_ORDER):
            @pl.when(used)
            def _():
                scale_copy(here, to).start()

    sent = sent + jnp.where(core != keeper, strips, 0)
    for used, _ in children(here, SCALE_ORDER):
        sent = sent + jnp.where((core == keeper) & used, strips, 0)

    @pl.when(core == keeper)
    def _():
        row = my_index * height
        own = codes.at[
            pl.ds(pl.multiple_of(row, ROWS), height),
            pl.ds(pl.multiple_of(core * width, LANES), width),
        ]
        pltpu.make_async_copy(mine, own, local_sem).start()

    low = core * half_depth
    top = low + half_depth - 1

    def source_of(q):
        i, j = q // plane, q % plane
        inside = low + (here[Z] - low + i + depth) % half_depth
        z = jnp.where(here[Z] >= top, top - i, jnp.where(here[Z] <= low, low + i, inside))
        return (z, (here[Y] + j // wide) % high, (here[X] + j % wide) % wide)

    def code_copy(source, k, to):
        part = code_slice(source, k)
        return pltpu.make_async_remote_copy(
            src_ref=part, dst_ref=part, send_sem=send_sem,
            recv_sem=recv_sem.at[chip_at(source) % sources, k],
            device_id=(core, to), device_id_type=MESH,
        )

    items = ITEMS.get(sizes)
    words = []
    if items:
        assert sorted(items) == [(q, k) for q in range(sources) for k in range(pieces + 1)]
        for start in range(0, len(items), WORD):
            chunk = items[start : start + WORD]
            words.append(sum((16 * q + k) << (7 * i) for i, (q, k) in enumerate(chunk)))

    def item_of(t):
        if not words:
            return t // (pieces + 1), t % (pieces + 1)
        word = jnp.int32(0)
        for i, held in enumerate(words):
            word = jnp.where(t // WORD == i, held, word)
        item = (word >> (7 * (t % WORD))) % 128
        return item // 16, item % 16

    def forward(t, sent):
        q, which = item_of(t)
        source = source_of(q)
        index = chip_at(source) % sources
        mine_too = chip_at(source) == chip

        for k, (order, column, _) in enumerate(PIECES):
            @pl.when((which == k) & jnp.logical_not(mine_too & (core == column)))
            def _():
                wait_bytes(code_slice(source, k), recv_sem.at[index, k])

            for_k = (which == k) & jnp.logical_not(mine_too)
            ways = children(source, order)

            @pl.when(for_k)
            def _():
                for used, to in ways:
                    @pl.when(used)
                    def _():
                        code_copy(source, k, to).start()

            for used, _ in ways:
                sent = sent + jnp.where(for_k & used, spans[k][1] * strips, 0)

        for_scale = (which == pieces) & jnp.logical_not(mine_too)
        ways = children(source, SCALE_ORDER)

        @pl.when(for_scale)
        def _():
            wait_bytes(scale_slice(source), recv_sem.at[index, pieces])
            for used, to in ways:
                @pl.when(used)
                def _():
                    scale_copy(source, to).start()

        for used, _ in ways:
            sent = sent + jnp.where(for_scale & used, strips, 0)
        return sent

    sent = lax.fori_loop(0, sources * (pieces + 1), forward, sent)

    @pl.when(core == keeper)
    def _():
        wait_bytes(mine, local_sem)

    most = broad
    while 2 * most <= broad * (codes.shape[0] // ROWS):
        most *= 2

    def drain(i, carry):
        wait_bytes(blocks(most), send_sem)
        return carry

    lax.fori_loop(0, sent // most, drain, 0)
    part = most // 2
    while part:
        @pl.when((sent // part) % 2 == 1)
        def _():
            wait_bytes(blocks(part), send_sem)

        part //= 2


def per_device(grid, master, gradient, first_moment, second_moment, max_norm, step_count):
    height, width = master.shape
    plane = grid[1] * grid[2]
    sources = grid[0] * plane // 2
    pieces = len(PIECES)
    kept = sources * height
    state = jax.ShapeDtypeStruct(master.shape, jnp.float32)
    held = pltpu.VMEM(master.shape, jnp.float32)
    narrow = pltpu.VMEM((height, LANES), jnp.bfloat16)
    dma = pltpu.SemaphoreType.DMA
    vmem = pl.BlockSpec(memory_space=pltpu.VMEM)
    smem = pl.BlockSpec(memory_space=pltpu.SMEM)
    hbm = pl.BlockSpec(memory_space=pltpu.HBM)
    free = pl.BlockSpec(memory_space=pl.ANY)
    state_in = [
        pltpu.with_memory_space_constraint(a, pltpu.HBM)
        for a in (master, gradient, first_moment, second_moment)
    ]
    results = pl.pallas_call(
        functools.partial(kernel, grid),
        out_shape=(
            state, state, state,
            jax.ShapeDtypeStruct((kept, 2 * width), jnp.bfloat16),
            jax.ShapeDtypeStruct((kept, 2 * width // BLOCK), jnp.bfloat16),
        ),
        in_specs=[smem, smem, hbm, hbm, hbm, hbm],
        out_specs=(vmem, vmem, vmem, free, vmem),
        scratch_shapes=[
            held, held, held, held,
            pltpu.VMEM((height, width), jnp.bfloat16),
            narrow,
            pltpu.VMEM((height, LANES), jnp.float32),
            narrow,
            pltpu.VMEM((max(2 * plane, ONE_STAGE), 1, LANES), jnp.float32),
            pltpu.VMEM((grid[0], 1, LANES), jnp.float32),
            dma((4,)), dma(()), dma(()), dma(()), dma(()), dma(()),
            dma((sources, pieces + 1)), dma(()),
        ],
        compiler_params=pltpu.CompilerParams(
            collective_id=0, has_side_effects=True, vmem_limit_bytes=KERNEL_VMEM
        ),
    )(max_norm, step_count, *state_in)
    return pl.pallas_call(
        flush,
        out_shape=tuple(jax.ShapeDtypeStruct(r.shape, r.dtype) for r in results),
        in_specs=[free] * len(results),
        out_specs=(hbm,) * len(results),
        scratch_shapes=[dma((len(results), PARTS))],
        compiler_params=pltpu.CompilerParams(vmem_limit_bytes=FLUSH_VMEM),
    )(*results)


def flush(*refs):
    count = len(refs) // 2
    sem = refs[-1]
    copies = []
    for i, (held, out) in enumerate(zip(refs[:count], refs[count:-1])):
        rows = held.shape[0] // PARTS
        for part in range(PARTS):
            span = pl.ds(part * rows, rows)
            copies.append(pltpu.make_async_copy(held.at[span], out.at[span], sem.at[i, part]))
    for copy in copies:
        copy.start()
    for copy in copies:
        copy.wait()


PARTS = 2
FLUSH_VMEM = 1024 * 1024


KERNEL_VMEM = 16 * 1024 * 1024


def solution(mesh):
    return jax.shard_map(
        functools.partial(per_device, grid_of(mesh)),
        mesh=mesh,
        in_specs=(
            P("shard", "pair"),
            P("shard", "pair"),
            P("shard", "pair"),
            P("shard", "pair"),
            P(),
            P(),
        ),
        out_specs=(
            P("shard", "pair"),
            P("shard", "pair"),
            P("shard", "pair"),
            P("pair", None),
            P("pair", None),
        ),
        check_vma=False,
    )
```

```python
import functools

import jax
import jax.numpy as jnp
from jax import lax
from jax.experimental import pallas as pl
from jax.experimental.pallas import tpu as pltpu
from jax.sharding import PartitionSpec as P

BLOCK = 32
LANES = 128

beta_first = 0.9
beta_second = 0.99
learn_rate = 0.01
decay_rate = 0.1
adam_eps = 1e-06
scale_floor = 0.25

MESH = pl.DeviceIdType.MESH
Z, Y, X = 0, 1, 2
PIECES = (
    ((Z, X, Y), 0, 5),
    ((Z, Y, X), 1, 6),
    ((X, Y, Z), 0, 5),
    ((Y, X, Z), 1, 2),
    ((Z, Y, X), 0, 6),
    ((Z, X, Y), 1, 8),
)
SCALE_ORDER = (Y, Z, X)
ROWS = 16
ITEMS = {
    (4, 2, 2): (
        (0, 1), (0, 4), (1, 3), (2, 3), (2, 2), (4, 1), (4, 0), (0, 5), (6, 1), (1, 2),
        (5, 1), (4, 6), (2, 6), (0, 0), (4, 5), (0, 6), (6, 3), (4, 4), (1, 5), (2, 4),
        (5, 2), (3, 3), (3, 6), (4, 2), (7, 1), (2, 1), (5, 0), (6, 2), (6, 0), (2, 0),
        (3, 2), (1, 0), (6, 5), (6, 6), (0, 3), (5, 5), (5, 6), (2, 5), (1, 6), (1, 4),
        (5, 3), (3, 5), (6, 4), (0, 2), (7, 3), (7, 2), (3, 0), (1, 1), (3, 1), (3, 4),
        (5, 4), (7, 0), (7, 6), (4, 3), (7, 5), (7, 4),
    ),
}
WORD = 4
ONE_STAGE = 32


def grid_of(mesh):
    count = mesh.shape["shard"]
    at = [d.coords for d in mesh.devices.reshape(mesh.shape["pair"], count)[0]]
    sizes = tuple(len({c[d] for c in at}) for d in (2, 1, 0))
    return sizes


def power(base, exponent):
    result = jnp.float32(1.0)
    for bit in range(31):
        factor = jnp.float32(base ** (2**bit))
        result = jnp.where((exponent >> bit) & 1 == 1, result * factor, result)
    return result


def kernel(
    grid, limit_ref, step_ref, master_hbm, gradient_hbm, first_hbm, second_hbm,
    new_master, new_first, new_second, codes, scales,
    master, gradient, first, second, mine, my_scales, wide_scales, their_scales,
    group_sums, line_sums,
    load_sem, sum_send, group_recv, line_recv, send_sem, peer_scale_recv, recv_sem, local_sem,
):
    sizes = grid
    depth, high, wide = sizes
    plane = high * wide
    half_depth = depth // 2
    sources = half_depth * plane
    height, width = mine.shape
    tiles = width // LANES
    pieces = len(PIECES)
    core = lax.axis_index("pair")
    chip = lax.axis_index("shard")
    here = (chip // plane, (chip // wide) % high, chip % wide)
    keeper = here[Z] // half_depth
    peer = 1 - core

    def chip_at(at):
        return (at[Z] * high + at[Y]) * wide + at[X]

    def wait_bytes(ref, sem):
        pltpu.make_async_copy(ref, ref, sem).wait()

    loads = [
        pltpu.make_async_copy(source, held, load_sem.at[i])
        for i, (source, held) in enumerate(
            ((gradient_hbm, gradient), (master_hbm, master), (first_hbm, first), (second_hbm, second))
        )
    ]
    loads[0].start()
    barrier = pltpu.get_barrier_semaphore()
    chips = depth * plane
    one_stage = 2 * chips <= ONE_STAGE
    if one_stage:
        group = 2 * chips
        my_place = core * chips + chip
    else:
        group = 2 * plane
        my_place = core * plane + here[Y] * wide + here[X]

    def member(place):
        if one_stage:
            return (place // chips, place % chips)
        return (place // plane, here[Z] * plane + place % plane)

    def greet(device):
        pl.semaphore_signal(barrier, inc=1, device_id=device, device_id_type=MESH)

    def greet_member(place, carry):
        @pl.when(place != my_place)
        def _():
            greet(member(place))

        return carry

    lax.fori_loop(0, group, greet_member, 0)
    greeted = group - 1
    if not one_stage:
        for other in range(depth):
            @pl.when(other != here[Z])
            def _():
                for side in range(2):
                    greet((side, chip_at((other, here[Y], here[X]))))

        greeted += 2 * (depth - 1)

    for load in loads[1:]:
        load.start()
    loads[0].wait()

    def square(i, totals):
        rows = gradient[pl.ds(pl.multiple_of(i * 8, 8), 8), :]
        totals = list(totals)
        for j in range(tiles):
            part = rows[:, j * LANES : (j + 1) * LANES]
            totals[j % 4] = totals[j % 4] + part * part
        return tuple(totals)

    totals = lax.fori_loop(
        0, height // 8, square, tuple(jnp.zeros((8, LANES), jnp.float32) for _ in range(4))
    )
    total = (totals[0] + totals[1]) + (totals[2] + totals[3])
    total = jnp.sum(total, axis=0, keepdims=True)

    one = jnp.ones((1, 1), jnp.float32)
    first_gain = one / (one - power(beta_first, step_ref[0]))
    second_gain = one / (one - power(beta_second, step_ref[0]))
    step_gain = jnp.broadcast_to(learn_rate * first_gain, (1, LANES))
    second_gain = jnp.broadcast_to(second_gain, (1, LANES))
    norm_limit = jnp.full((1, 1), limit_ref[0], jnp.float32)

    pl.semaphore_wait(barrier, greeted)

    def exchange(value, buffer, place, count, device_of, recv):
        buffer[place] = value

        def copy(other):
            return pltpu.make_async_remote_copy(
                src_ref=buffer.at[place], dst_ref=buffer.at[place],
                send_sem=sum_send, recv_sem=recv,
                device_id=device_of(other), device_id_type=MESH,
            )

        def send(other, carry):
            @pl.when(other != place)
            def _():
                copy(other).start()

            return carry

        lax.fori_loop(0, count, send, 0)
        others = buffer.at[pl.ds(0, count - 1)]
        wait_bytes(others, recv)
        wait_bytes(others, sum_send)
        return jnp.sum(buffer[pl.ds(0, count)], axis=0)

    total = exchange(total, group_sums, my_place, group, member, group_recv)
    if not one_stage:
        total = exchange(
            total, line_sums, here[Z], depth,
            lambda other: (core, chip_at((other, here[Y], here[X]))), line_recv,
        )
    squares = jnp.sum(total, axis=1, keepdims=True)
    clip_factor = norm_limit / jnp.maximum(jnp.sqrt(squares), norm_limit)
    clip_factor = jnp.broadcast_to(clip_factor, (1, LANES))
    clip_first = (1.0 - beta_first) * clip_factor
    clip_second = (1.0 - beta_second) * clip_factor * clip_factor
    for load in loads[1:]:
        load.wait()

    def children(source, order):
        last = jnp.int32(-1)
        for i, dim in enumerate(order):
            last = jnp.where(here[dim] != source[dim], i, last)
        ways = []
        for i, dim in enumerate(order):
            if sizes[dim] == 2:
                there = list(here)
                there[dim] = 1 - here[dim]
                ways.append((last < i, chip_at(there)))
            elif sizes[dim] > 2:
                for step in (1, -1):
                    there = list(here)
                    there[dim] = here[dim] + step
                    inside = (there[dim] >= 0) & (there[dim] < sizes[dim])
                    away = (here[dim] - source[dim]) * step > 0
                    ways.append((inside & ((last < i) | ((last == i) & away)), chip_at(there)))
        return ways

    spans = []
    at = [0, 0]
    for _, column, share in PIECES:
        spans.append((at[column], tiles * share // 16))
        at[column] += spans[-1][1]
    assert at == [tiles, tiles]

    def code_part(source, column, start, size, top_row=0, rows=height):
        row = (chip_at(source) % sources) * height + top_row
        lane = column * width + start * LANES
        return codes.at[pl.ds(pl.multiple_of(row, ROWS), rows), pl.ds(lane, size * LANES)]

    def code_slice(source, k):
        return code_part(source, PIECES[k][1], *spans[k])

    def scale_slice(source):
        row = (chip_at(source) % sources) * height
        return scales.at[pl.ds(pl.multiple_of(row, 16), height), :]

    strips = height // ROWS
    broad = 1
    while 2 * broad <= 2 * tiles:
        broad *= 2

    def blocks(count):
        if count <= broad:
            return codes.at[pl.ds(0, ROWS), pl.ds(0, count * LANES)]
        return codes.at[pl.ds(0, count // broad * ROWS), pl.ds(0, broad * LANES)]

    my_index = chip % sources

    def own_copy(column, k, start, size, top_row, rows, to):
        return pltpu.make_async_remote_copy(
            src_ref=mine.at[pl.ds(top_row, rows), pl.ds(start * LANES, size * LANES)],
            dst_ref=code_part(here, column, start, size, top_row, rows),
            send_sem=send_sem, recv_sem=recv_sem.at[my_index, k],
            device_id=(keeper, to), device_id_type=MESH,
        )

    lane = lax.broadcasted_iota(jnp.int32, (1, LANES), 1)
    spread_row = lax.broadcasted_iota(jnp.int32, (LANES, LANES), 0)
    spread_column = lax.broadcasted_iota(jnp.int32, (LANES, LANES), 1)
    spread = (spread_row == spread_column // BLOCK * BLOCK).astype(jnp.float32).astype(jnp.bfloat16)
    per_tile = LANES // BLOCK
    assert tiles <= BLOCK

    def tile(j, top_row=0, rows=height):
        band = pl.ds(top_row, rows)
        where = (band, pl.ds(pl.multiple_of(j * LANES, LANES), LANES))
        weight = master[where]
        slope = gradient[where]
        moment = beta_first * first[where] + clip_first * slope
        power_moment = beta_second * second[where] + clip_second * (slope * slope)
        new_first[where] = moment
        new_second[where] = power_moment
        scaled = power_moment * second_gain
        root = scaled * lax.rsqrt(scaled)
        weight = (1.0 - learn_rate * decay_rate) * weight - step_gain * moment / (root + adam_eps)
        new_master[where] = weight
        largest = jnp.abs(weight)
        shift = BLOCK // 2
        while shift:
            largest = jnp.maximum(largest, pltpu.roll(largest, LANES - shift, axis=1))
            shift //= 2
        scale = jnp.maximum(largest, scale_floor).astype(jnp.bfloat16)
        scale = jnp.dot(scale, spread, preferred_element_type=jnp.float32)
        mine[where] = (weight / scale).astype(jnp.bfloat16)
        wide_scales[band, :] = jnp.where(lane % BLOCK == j, scale, wide_scales[band, :])

    wide_scales[...] = jnp.zeros_like(wide_scales)
    sent = jnp.int32(0)
    for c in range(2):
        def own_pieces(sent):
            for k, (order, column, _) in enumerate(PIECES):
                if column != c:
                    continue
                start, size = spans[k]
                parts = [(0, size, 0, height)]
                if start == 0:
                    cuts = [0, 1, 3, size] if size > 3 else [0, 1, size]
                    parts = [(a, b - a, 0, height) for a, b in zip(cuts, cuts[1:])]
                for offset, part, top_row, rows in parts:
                    begin = start + offset

                    def one_tile(j, carry):
                        tile(j, top_row, rows)
                        return carry

                    lax.fori_loop(begin, begin + part, one_tile, 0)
                    amount = part * rows // ROWS
                    for used, to in children(here, order):
                        @pl.when(used)
                        def _():
                            own_copy(c, k, begin, part, top_row, rows, to).start()

                        sent = sent + jnp.where(used, amount, 0)

                    @pl.when(c != keeper)
                    def _():
                        own_copy(c, k, begin, part, top_row, rows, chip).start()

                    sent = sent + jnp.where(c != keeper, amount, 0)
            return sent

        sent = lax.cond(core == c, own_pieces, lambda s: s, sent)

    place_row = spread_row % BLOCK
    target = (core * tiles + place_row) * per_tile + spread_row // BLOCK
    pick = ((place_row < tiles) & (spread_column == target)).astype(jnp.float32)
    placed = jnp.dot(
        wide_scales[...].astype(jnp.bfloat16), pick.astype(jnp.bfloat16),
        preferred_element_type=jnp.float32,
    )
    my_scales[...] = placed.astype(jnp.bfloat16)
    peer_scales = pltpu.make_async_remote_copy(
        src_ref=my_scales, dst_ref=their_scales, send_sem=send_sem,
        recv_sem=peer_scale_recv, device_id=(peer, chip), device_id_type=MESH,
    )

    def scale_copy(source, to):
        return pltpu.make_async_remote_copy(
            src_ref=scale_slice(source), dst_ref=scale_slice(source),
            send_sem=send_sem, recv_sem=recv_sem.at[chip_at(source) % sources, pieces],
            device_id=(core, to), device_id_type=MESH,
        )

    @pl.when(core != keeper)
    def _():
        peer_scales.start()

    @pl.when(core == keeper)
    def _():
        peer_scales.wait_recv()
        merged = my_scales[...] + their_scales[...]
        row = pl.ds(pl.multiple_of(my_index * height, 16), height)
        scales[row, :] = merged
        for used, to in children(here, SCALE_ORDER):
            @pl.when(used)
            def _():
                scale_copy(here, to).start()

    sent = sent + jnp.where(core != keeper, strips, 0)
    for used, _ in children(here, SCALE_ORDER):
        sent = sent + jnp.where((core == keeper) & used, strips, 0)

    @pl.when(core == keeper)
    def _():
        row = my_index * height
        own = codes.at[
            pl.ds(pl.multiple_of(row, ROWS), height),
            pl.ds(pl.multiple_of(core * width, LANES), width),
        ]
        pltpu.make_async_copy(mine, own, local_sem).start()

    low = core * half_depth
    top = low + half_depth - 1

    def source_of(q):
        i, j = q // plane, q % plane
        inside = low + (here[Z] - low + i + depth) % half_depth
        z = jnp.where(here[Z] >= top, top - i, jnp.where(here[Z] <= low, low + i, inside))
        return (z, (here[Y] + j // wide) % high, (here[X] + j % wide) % wide)

    def code_copy(source, k, to):
        part = code_slice(source, k)
        return pltpu.make_async_remote_copy(
            src_ref=part, dst_ref=part, send_sem=send_sem,
            recv_sem=recv_sem.at[chip_at(source) % sources, k],
            device_id=(core, to), device_id_type=MESH,
        )

    items = ITEMS.get(sizes)
    words = []
    if items:
        assert sorted(items) == [(q, k) for q in range(sources) for k in range(pieces + 1)]
        for start in range(0, len(items), WORD):
            chunk = items[start : start + WORD]
            words.append(sum((16 * q + k) << (7 * i) for i, (q, k) in enumerate(chunk)))

    def item_of(t):
        if not words:
            return t // (pieces + 1), t % (pieces + 1)
        word = jnp.int32(0)
        for i, held in enumerate(words):
            word = jnp.where(t // WORD == i, held, word)
        item = (word >> (7 * (t % WORD))) % 128
        return item // 16, item % 16

    def forward(t, sent):
        q, which = item_of(t)
        source = source_of(q)
        index = chip_at(source) % sources
        mine_too = chip_at(source) == chip

        for k, (order, column, _) in enumerate(PIECES):
            @pl.when((which == k) & jnp.logical_not(mine_too & (core == column)))
            def _():
                wait_bytes(code_slice(source, k), recv_sem.at[index, k])

            for_k = (which == k) & jnp.logical_not(mine_too)
            ways = children(source, order)

            @pl.when(for_k)
            def _():
                for used, to in ways:
                    @pl.when(used)
                    def _():
                        code_copy(source, k, to).start()

            for used, _ in ways:
                sent = sent + jnp.where(for_k & used, spans[k][1] * strips, 0)

        for_scale = (which == pieces) & jnp.logical_not(mine_too)
        ways = children(source, SCALE_ORDER)

        @pl.when(for_scale)
        def _():
            wait_bytes(scale_slice(source), recv_sem.at[index, pieces])
            for used, to in ways:
                @pl.when(used)
                def _():
                    scale_copy(source, to).start()

        for used, _ in ways:
            sent = sent + jnp.where(for_scale & used, strips, 0)
        return sent

    sent = lax.fori_loop(0, sources * (pieces + 1), forward, sent)

    @pl.when(core == keeper)
    def _():
        wait_bytes(mine, local_sem)

    most = broad
    while 2 * most <= broad * (codes.shape[0] // ROWS):
        most *= 2

    def drain(i, carry):
        wait_bytes(blocks(most), send_sem)
        return carry

    lax.fori_loop(0, sent // most, drain, 0)
    part = most // 2
    while part:
        @pl.when((sent // part) % 2 == 1)
        def _():
            wait_bytes(blocks(part), send_sem)

        part //= 2


def per_device(grid, master, gradient, first_moment, second_moment, max_norm, step_count):
    height, width = master.shape
    plane = grid[1] * grid[2]
    sources = grid[0] * plane // 2
    pieces = len(PIECES)
    kept = sources * height
    state = jax.ShapeDtypeStruct(master.shape, jnp.float32)
    held = pltpu.VMEM(master.shape, jnp.float32)
    narrow = pltpu.VMEM((height, LANES), jnp.bfloat16)
    dma = pltpu.SemaphoreType.DMA
    vmem = pl.BlockSpec(memory_space=pltpu.VMEM)
    smem = pl.BlockSpec(memory_space=pltpu.SMEM)
    hbm = pl.BlockSpec(memory_space=pltpu.HBM)
    free = pl.BlockSpec(memory_space=pl.ANY)
    state_in = [
        pltpu.with_memory_space_constraint(a, pltpu.HBM)
        for a in (master, gradient, first_moment, second_moment)
    ]
    results = pl.pallas_call(
        functools.partial(kernel, grid),
        out_shape=(
            state, state, state,
            jax.ShapeDtypeStruct((kept, 2 * width), jnp.bfloat16),
            jax.ShapeDtypeStruct((kept, 2 * width // BLOCK), jnp.bfloat16),
        ),
        in_specs=[smem, smem, hbm, hbm, hbm, hbm],
        out_specs=(vmem, vmem, vmem, free, vmem),
        scratch_shapes=[
            held, held, held, held,
            pltpu.VMEM((height, width), jnp.bfloat16),
            narrow,
            pltpu.VMEM((height, LANES), jnp.float32),
            narrow,
            pltpu.VMEM((max(2 * plane, ONE_STAGE), 1, LANES), jnp.float32),
            pltpu.VMEM((grid[0], 1, LANES), jnp.float32),
            dma((4,)), dma(()), dma(()), dma(()), dma(()), dma(()),
            dma((sources, pieces + 1)), dma(()),
        ],
        compiler_params=pltpu.CompilerParams(
            collective_id=0, has_side_effects=True, vmem_limit_bytes=KERNEL_VMEM
        ),
    )(max_norm, step_count, *state_in)
    return pl.pallas_call(
        flush,
        out_shape=tuple(jax.ShapeDtypeStruct(r.shape, r.dtype) for r in results),
        in_specs=[free] * len(results),
        out_specs=(hbm,) * len(results),
        scratch_shapes=[dma((len(results), PARTS))],
        compiler_params=pltpu.CompilerParams(vmem_limit_bytes=FLUSH_VMEM),
    )(*results)


def flush(*refs):
    count = len(refs) // 2
    sem = refs[-1]
    copies = []
    for i, (held, out) in enumerate(zip(refs[:count], refs[count:-1])):
        rows = held.shape[0] // PARTS
        for part in range(PARTS):
            span = pl.ds(part * rows, rows)
            copies.append(pltpu.make_async_copy(held.at[span], out.at[span], sem.at[i, part]))
    for copy in copies:
        copy.start()
    for copy in copies:
        copy.wait()


PARTS = 2
FLUSH_VMEM = 1024 * 1024


KERNEL_VMEM = 16 * 1024 * 1024


def solution(mesh):
    return jax.shard_map(
        functools.partial(per_device, grid_of(mesh)),
        mesh=mesh,
        in_specs=(
            P("shard", "pair"),
            P("shard", "pair"),
            P("shard", "pair"),
            P("shard", "pair"),
            P(),
            P(),
        ),
        out_specs=(
            P("shard", "pair"),
            P("shard", "pair"),
            P("shard", "pair"),
            P("pair", None),
            P("pair", None),
        ),
        check_vma=False,
    )
```

```python
import functools

import jax
import jax.numpy as jnp
from jax import lax
from jax.experimental import pallas as pl
from jax.experimental.pallas import tpu as pltpu
from jax.sharding import PartitionSpec as P

BLOCK = 32
LANES = 128

beta_first = 0.9
beta_second = 0.99
learn_rate = 0.01
decay_rate = 0.1
adam_eps = 1e-06
scale_floor = 0.25

MESH = pl.DeviceIdType.MESH
Z, Y, X = 0, 1, 2
PIECES = (
    ((Z, X, Y), 0, 5),
    ((Z, Y, X), 1, 6),
    ((X, Y, Z), 0, 5),
    ((Y, X, Z), 1, 2),
    ((Z, Y, X), 0, 6),
    ((Z, X, Y), 1, 8),
)
SCALE_ORDER = (Y, Z, X)
ROWS = 16
ITEMS = {
    (4, 2, 2): (
        (0, 0), (0, 1), (4, 1), (0, 4), (4, 0), (0, 5), (4, 5), (2, 2), (2, 6), (0, 6),
        (2, 3), (4, 4), (3, 3), (1, 2), (3, 2), (1, 0), (6, 6), (2, 0), (5, 0), (1, 5),
        (5, 5), (7, 3), (1, 3), (2, 1), (0, 2), (1, 1), (5, 1), (2, 4), (6, 0), (1, 4),
        (5, 2), (6, 3), (4, 3), (3, 0), (7, 6), (6, 4), (3, 6), (4, 6), (5, 3), (3, 1),
        (4, 2), (6, 1), (2, 5), (7, 0), (7, 2), (6, 2), (3, 4), (5, 6), (6, 5), (1, 6),
        (3, 5), (7, 4), (5, 4), (0, 3), (7, 5), (7, 1),
    ),
}
WORD = 4
ONE_STAGE = 32


def grid_of(mesh):
    count = mesh.shape["shard"]
    at = [d.coords for d in mesh.devices.reshape(mesh.shape["pair"], count)[0]]
    sizes = tuple(len({c[d] for c in at}) for d in (2, 1, 0))
    return sizes


def power(base, exponent):
    result = jnp.float32(1.0)
    for bit in range(31):
        factor = jnp.float32(base ** (2**bit))
        result = jnp.where((exponent >> bit) & 1 == 1, result * factor, result)
    return result


def kernel(
    grid, limit_ref, step_ref, master_hbm, gradient_hbm, first_hbm, second_hbm,
    new_master, new_first, new_second, codes, scales,
    master, gradient, first, second, mine, my_scales, wide_scales, their_scales,
    group_sums, line_sums,
    load_sem, sum_send, group_recv, line_recv, send_sem, peer_scale_recv, recv_sem, local_sem,
):
    sizes = grid
    depth, high, wide = sizes
    plane = high * wide
    half_depth = depth // 2
    sources = half_depth * plane
    height, width = mine.shape
    tiles = width // LANES
    pieces = len(PIECES)
    core = lax.axis_index("pair")
    chip = lax.axis_index("shard")
    here = (chip // plane, (chip // wide) % high, chip % wide)
    keeper = here[Z] // half_depth
    peer = 1 - core

    def chip_at(at):
        return (at[Z] * high + at[Y]) * wide + at[X]

    def wait_bytes(ref, sem):
        pltpu.make_async_copy(ref, ref, sem).wait()

    loads = [
        pltpu.make_async_copy(source, held, load_sem.at[i])
        for i, (source, held) in enumerate(
            ((gradient_hbm, gradient), (master_hbm, master), (first_hbm, first), (second_hbm, second))
        )
    ]
    loads[0].start()
    barrier = pltpu.get_barrier_semaphore()
    chips = depth * plane
    one_stage = 2 * chips <= ONE_STAGE
    if one_stage:
        group = 2 * chips
        my_place = core * chips + chip
    else:
        group = 2 * plane
        my_place = core * plane + here[Y] * wide + here[X]

    def member(place):
        if one_stage:
            return (place // chips, place % chips)
        return (place // plane, here[Z] * plane + place % plane)

    def greet(device):
        pl.semaphore_signal(barrier, inc=1, device_id=device, device_id_type=MESH)

    def greet_member(place, carry):
        @pl.when(place != my_place)
        def _():
            greet(member(place))

        return carry

    lax.fori_loop(0, group, greet_member, 0)
    greeted = group - 1
    if not one_stage:
        for other in range(depth):
            @pl.when(other != here[Z])
            def _():
                for side in range(2):
                    greet((side, chip_at((other, here[Y], here[X]))))

        greeted += 2 * (depth - 1)

    for load in loads[1:]:
        load.start()
    loads[0].wait()

    def square(i, totals):
        rows = gradient[pl.ds(pl.multiple_of(i * 8, 8), 8), :]
        totals = list(totals)
        for j in range(tiles):
            part = rows[:, j * LANES : (j + 1) * LANES]
            totals[j % 4] = totals[j % 4] + part * part
        return tuple(totals)

    totals = lax.fori_loop(
        0, height // 8, square, tuple(jnp.zeros((8, LANES), jnp.float32) for _ in range(4))
    )
    total = (totals[0] + totals[1]) + (totals[2] + totals[3])
    total = jnp.sum(total, axis=0, keepdims=True)

    one = jnp.ones((1, 1), jnp.float32)
    first_gain = one / (one - power(beta_first, step_ref[0]))
    second_gain = one / (one - power(beta_second, step_ref[0]))
    step_gain = jnp.broadcast_to(learn_rate * first_gain, (1, LANES))
    second_gain = jnp.broadcast_to(second_gain, (1, LANES))
    norm_limit = jnp.full((1, 1), limit_ref[0], jnp.float32)

    pl.semaphore_wait(barrier, greeted)

    def exchange(value, buffer, place, count, device_of, recv):
        buffer[place] = value

        def copy(other):
            return pltpu.make_async_remote_copy(
                src_ref=buffer.at[place], dst_ref=buffer.at[place],
                send_sem=sum_send, recv_sem=recv,
                device_id=device_of(other), device_id_type=MESH,
            )

        def send(other, carry):
            @pl.when(other != place)
            def _():
                copy(other).start()

            return carry

        lax.fori_loop(0, count, send, 0)
        others = buffer.at[pl.ds(0, count - 1)]
        wait_bytes(others, recv)
        wait_bytes(others, sum_send)
        return jnp.sum(buffer[pl.ds(0, count)], axis=0)

    total = exchange(total, group_sums, my_place, group, member, group_recv)
    if not one_stage:
        total = exchange(
            total, line_sums, here[Z], depth,
            lambda other: (core, chip_at((other, here[Y], here[X]))), line_recv,
        )
    squares = jnp.sum(total, axis=1, keepdims=True)
    clip_factor = norm_limit / jnp.maximum(jnp.sqrt(squares), norm_limit)
    clip_factor = jnp.broadcast_to(clip_factor, (1, LANES))
    clip_first = (1.0 - beta_first) * clip_factor
    clip_second = (1.0 - beta_second) * clip_factor * clip_factor
    for load in loads[1:]:
        load.wait()

    def children(source, order):
        last = jnp.int32(-1)
        for i, dim in enumerate(order):
            last = jnp.where(here[dim] != source[dim], i, last)
        ways = []
        for i, dim in enumerate(order):
            if sizes[dim] == 2:
                there = list(here)
                there[dim] = 1 - here[dim]
                ways.append((last < i, chip_at(there)))
            elif sizes[dim] > 2:
                for step in (1, -1):
                    there = list(here)
                    there[dim] = here[dim] + step
                    inside = (there[dim] >= 0) & (there[dim] < sizes[dim])
                    away = (here[dim] - source[dim]) * step > 0
                    ways.append((inside & ((last < i) | ((last == i) & away)), chip_at(there)))
        return ways

    spans = []
    at = [0, 0]
    for _, column, share in PIECES:
        spans.append((at[column], tiles * share // 16))
        at[column] += spans[-1][1]
    assert at == [tiles, tiles]

    def code_part(source, column, start, size):
        row = (chip_at(source) % sources) * height
        lane = column * width + start * LANES
        return codes.at[pl.ds(pl.multiple_of(row, ROWS), height), pl.ds(lane, size * LANES)]

    def code_slice(source, k):
        return code_part(source, PIECES[k][1], *spans[k])

    def scale_slice(source):
        row = (chip_at(source) % sources) * height
        return scales.at[pl.ds(pl.multiple_of(row, 16), height), :]

    strips = height // ROWS
    broad = 1
    while 2 * broad <= 2 * tiles:
        broad *= 2

    def blocks(count):
        if count <= broad:
            return codes.at[pl.ds(0, ROWS), pl.ds(0, count * LANES)]
        return codes.at[pl.ds(0, count // broad * ROWS), pl.ds(0, broad * LANES)]

    my_index = chip % sources

    def own_copy(column, k, start, size, to):
        return pltpu.make_async_remote_copy(
            src_ref=mine.at[:, pl.ds(start * LANES, size * LANES)],
            dst_ref=code_part(here, column, start, size),
            send_sem=send_sem, recv_sem=recv_sem.at[my_index, k],
            device_id=(keeper, to), device_id_type=MESH,
        )

    lane = lax.broadcasted_iota(jnp.int32, (1, LANES), 1)
    spread_row = lax.broadcasted_iota(jnp.int32, (LANES, LANES), 0)
    spread_column = lax.broadcasted_iota(jnp.int32, (LANES, LANES), 1)
    spread = (spread_row == spread_column // BLOCK * BLOCK).astype(jnp.float32).astype(jnp.bfloat16)
    per_tile = LANES // BLOCK
    assert tiles <= BLOCK

    def tile(j):
        where = (slice(None), pl.ds(pl.multiple_of(j * LANES, LANES), LANES))
        weight = master[where]
        slope = gradient[where]
        moment = beta_first * first[where] + clip_first * slope
        power_moment = beta_second * second[where] + clip_second * (slope * slope)
        new_first[where] = moment
        new_second[where] = power_moment
        scaled = power_moment * second_gain
        root = scaled * lax.rsqrt(scaled)
        weight = (1.0 - learn_rate * decay_rate) * weight - step_gain * moment / (root + adam_eps)
        new_master[where] = weight
        largest = jnp.abs(weight)
        shift = BLOCK // 2
        while shift:
            largest = jnp.maximum(largest, pltpu.roll(largest, LANES - shift, axis=1))
            shift //= 2
        scale = jnp.maximum(largest, scale_floor).astype(jnp.bfloat16)
        scale = jnp.dot(scale, spread, preferred_element_type=jnp.float32)
        mine[where] = (weight / scale).astype(jnp.bfloat16)
        wide_scales[...] = jnp.where(lane % BLOCK == j, scale, wide_scales[...])

    wide_scales[...] = jnp.zeros_like(wide_scales)
    parts = ([], [])
    for k, (_, column, _) in enumerate(PIECES):
        start, size = spans[k]
        cuts = [0, size]
        if start == 0:
            cuts = [0, 1, 3, size] if size > 3 else [0, 1, size]
        parts[column].extend((k, start + a, b - a) for a, b in zip(cuts, cuts[1:]))
    my_ways = {order: children(here, order) for order, _, _ in PIECES}

    def one_tile(j, carry):
        tile(j)
        return carry

    def send_part(p, carry):
        begin, end = jnp.int32(0), jnp.int32(0)
        for c in range(2):
            for i, (_, first_tile, count) in enumerate(parts[c]):
                at = (core == c) & (p == i)
                begin = jnp.where(at, first_tile, begin)
                end = jnp.where(at, first_tile + count, end)
        lax.fori_loop(begin, end, one_tile, 0)

        for c in range(2):
            for i, (k, first_tile, count) in enumerate(parts[c]):
                @pl.when((core == c) & (p == i))
                def _():
                    for used, to in my_ways[PIECES[k][0]]:
                        @pl.when(used)
                        def _():
                            own_copy(c, k, first_tile, count, to).start()

                    @pl.when(c != keeper)
                    def _():
                        own_copy(c, k, first_tile, count, chip).start()

        return carry

    lax.fori_loop(0, max(len(p) for p in parts), send_part, 0)
    sent = jnp.int32(0)
    for k, (order, column, _) in enumerate(PIECES):
        amount = spans[k][1] * strips
        for used, _ in my_ways[order]:
            sent = sent + jnp.where((core == column) & used, amount, 0)
        sent = sent + jnp.where((core == column) & (column != keeper), amount, 0)

    place_row = spread_row % BLOCK
    target = (core * tiles + place_row) * per_tile + spread_row // BLOCK
    pick = ((place_row < tiles) & (spread_column == target)).astype(jnp.float32)
    placed = jnp.dot(
        wide_scales[...].astype(jnp.bfloat16), pick.astype(jnp.bfloat16),
        preferred_element_type=jnp.float32,
    )
    my_scales[...] = placed.astype(jnp.bfloat16)
    peer_scales = pltpu.make_async_remote_copy(
        src_ref=my_scales, dst_ref=their_scales, send_sem=send_sem,
        recv_sem=peer_scale_recv, device_id=(peer, chip), device_id_type=MESH,
    )

    def scale_copy(source, to):
        return pltpu.make_async_remote_copy(
            src_ref=scale_slice(source), dst_ref=scale_slice(source),
            send_sem=send_sem, recv_sem=recv_sem.at[chip_at(source) % sources, pieces],
            device_id=(core, to), device_id_type=MESH,
        )

    @pl.when(core != keeper)
    def _():
        peer_scales.start()

    @pl.when(core == keeper)
    def _():
        peer_scales.wait_recv()
        merged = my_scales[...] + their_scales[...]
        row = pl.ds(pl.multiple_of(my_index * height, 16), height)
        scales[row, :] = merged
        for used, to in children(here, SCALE_ORDER):
            @pl.when(used)
            def _():
                scale_copy(here, to).start()

    sent = sent + jnp.where(core != keeper, strips, 0)
    for used, _ in children(here, SCALE_ORDER):
        sent = sent + jnp.where((core == keeper) & used, strips, 0)

    @pl.when(core == keeper)
    def _():
        row = my_index * height
        own = codes.at[
            pl.ds(pl.multiple_of(row, ROWS), height),
            pl.ds(pl.multiple_of(core * width, LANES), width),
        ]
        pltpu.make_async_copy(mine, own, local_sem).start()

    low = core * half_depth
    top = low + half_depth - 1

    def source_of(q):
        i, j = q // plane, q % plane
        inside = low + (here[Z] - low + i + depth) % half_depth
        z = jnp.where(here[Z] >= top, top - i, jnp.where(here[Z] <= low, low + i, inside))
        return (z, (here[Y] + j // wide) % high, (here[X] + j % wide) % wide)

    def code_copy(source, k, to):
        part = code_slice(source, k)
        return pltpu.make_async_remote_copy(
            src_ref=part, dst_ref=part, send_sem=send_sem,
            recv_sem=recv_sem.at[chip_at(source) % sources, k],
            device_id=(core, to), device_id_type=MESH,
        )

    items = ITEMS.get(sizes)
    words = []
    if items:
        assert sorted(items) == [(q, k) for q in range(sources) for k in range(pieces + 1)]
        for start in range(0, len(items), WORD):
            chunk = items[start : start + WORD]
            words.append(sum((16 * q + k) << (7 * i) for i, (q, k) in enumerate(chunk)))

    def item_of(t):
        if not words:
            return t // (pieces + 1), t % (pieces + 1)
        word = jnp.int32(0)
        for i, held in enumerate(words):
            word = jnp.where(t // WORD == i, held, word)
        item = (word >> (7 * (t % WORD))) % 128
        return item // 16, item % 16

    def forward(t, carry):
        q, which = item_of(t)
        source = source_of(q)
        index = chip_at(source) % sources
        mine_too = chip_at(source) == chip

        for k, (order, column, _) in enumerate(PIECES):
            @pl.when((which == k) & jnp.logical_not(mine_too & (core == column)))
            def _():
                wait_bytes(code_slice(source, k), recv_sem.at[index, k])

            @pl.when((which == k) & jnp.logical_not(mine_too))
            def _():
                for used, to in children(source, order):
                    @pl.when(used)
                    def _():
                        code_copy(source, k, to).start()

        @pl.when((which == pieces) & jnp.logical_not(mine_too))
        def _():
            wait_bytes(scale_slice(source), recv_sem.at[index, pieces])
            for used, to in children(source, SCALE_ORDER):
                @pl.when(used)
                def _():
                    scale_copy(source, to).start()

        return carry

    def passed(q, sent):
        source = source_of(q)
        others = chip_at(source) != chip
        orders = [(order, spans[k][1] * strips) for k, (order, _, _) in enumerate(PIECES)]
        for order in sorted({order for order, _ in orders} | {SCALE_ORDER}):
            amount = sum(a for o, a in orders if o == order) + (order == SCALE_ORDER) * strips
            for used, _ in children(source, order):
                sent = sent + jnp.where(others & used, amount, 0)
        return sent

    sent = lax.fori_loop(0, sources, passed, sent)
    lax.fori_loop(0, sources * (pieces + 1), forward, 0)

    @pl.when(core == keeper)
    def _():
        wait_bytes(mine, local_sem)

    most = broad
    while 2 * most <= broad * (codes.shape[0] // ROWS):
        most *= 2

    def drain(i, carry):
        wait_bytes(blocks(most), send_sem)
        return carry

    lax.fori_loop(0, sent // most, drain, 0)
    part = most // 2
    while part:
        @pl.when((sent // part) % 2 == 1)
        def _():
            wait_bytes(blocks(part), send_sem)

        part //= 2


def per_device(grid, master, gradient, first_moment, second_moment, max_norm, step_count):
    height, width = master.shape
    plane = grid[1] * grid[2]
    sources = grid[0] * plane // 2
    pieces = len(PIECES)
    kept = sources * height
    state = jax.ShapeDtypeStruct(master.shape, jnp.float32)
    held = pltpu.VMEM(master.shape, jnp.float32)
    narrow = pltpu.VMEM((height, LANES), jnp.bfloat16)
    dma = pltpu.SemaphoreType.DMA
    vmem = pl.BlockSpec(memory_space=pltpu.VMEM)
    smem = pl.BlockSpec(memory_space=pltpu.SMEM)
    hbm = pl.BlockSpec(memory_space=pltpu.HBM)
    free = pl.BlockSpec(memory_space=pl.ANY)
    state_in = [
        pltpu.with_memory_space_constraint(a, pltpu.HBM)
        for a in (master, gradient, first_moment, second_moment)
    ]
    results = pl.pallas_call(
        functools.partial(kernel, grid),
        out_shape=(
            state, state, state,
            jax.ShapeDtypeStruct((kept, 2 * width), jnp.bfloat16),
            jax.ShapeDtypeStruct((kept, 2 * width // BLOCK), jnp.bfloat16),
        ),
        in_specs=[smem, smem, hbm, hbm, hbm, hbm],
        out_specs=(vmem, vmem, vmem, free, vmem),
        scratch_shapes=[
            held, held, held, held,
            pltpu.VMEM((height, width), jnp.bfloat16),
            narrow,
            pltpu.VMEM((height, LANES), jnp.float32),
            narrow,
            pltpu.VMEM((max(2 * plane, ONE_STAGE), 1, LANES), jnp.float32),
            pltpu.VMEM((grid[0], 1, LANES), jnp.float32),
            dma((4,)), dma(()), dma(()), dma(()), dma(()), dma(()),
            dma((sources, pieces + 1)), dma(()),
        ],
        compiler_params=pltpu.CompilerParams(
            collective_id=0, has_side_effects=True, vmem_limit_bytes=KERNEL_VMEM
        ),
    )(max_norm, step_count, *state_in)
    return pl.pallas_call(
        flush,
        out_shape=tuple(jax.ShapeDtypeStruct(r.shape, r.dtype) for r in results),
        in_specs=[free] * len(results),
        out_specs=(hbm,) * len(results),
        scratch_shapes=[dma((len(results), PARTS))],
        compiler_params=pltpu.CompilerParams(vmem_limit_bytes=FLUSH_VMEM),
    )(*results)


def flush(*refs):
    count = len(refs) // 2
    sem = refs[-1]
    copies = []
    for i, (held, out) in enumerate(zip(refs[:count], refs[count:-1])):
        rows = held.shape[0] // PARTS
        for part in range(PARTS):
            span = pl.ds(part * rows, rows)
            copies.append(pltpu.make_async_copy(held.at[span], out.at[span], sem.at[i, part]))
    for copy in copies:
        copy.start()
    for copy in copies:
        copy.wait()


PARTS = 2
FLUSH_VMEM = 1024 * 1024


KERNEL_VMEM = 16 * 1024 * 1024


def solution(mesh):
    return jax.shard_map(
        functools.partial(per_device, grid_of(mesh)),
        mesh=mesh,
        in_specs=(
            P("shard", "pair"),
            P("shard", "pair"),
            P("shard", "pair"),
            P("shard", "pair"),
            P(),
            P(),
        ),
        out_specs=(
            P("shard", "pair"),
            P("shard", "pair"),
            P("shard", "pair"),
            P("pair", None),
            P("pair", None),
        ),
        check_vma=False,
    )
```

```python
import functools

import jax
import jax.numpy as jnp
from jax import lax
from jax.experimental import pallas as pl
from jax.experimental.pallas import tpu as pltpu
from jax.sharding import PartitionSpec as P

BLOCK = 32
LANES = 128

beta_first = 0.9
beta_second = 0.99
learn_rate = 0.01
decay_rate = 0.1
adam_eps = 1e-06
scale_floor = 0.25

MESH = pl.DeviceIdType.MESH
Z, Y, X = 0, 1, 2
PIECES = (
    ((Z, X, Y), 0, 5),
    ((Z, Y, X), 1, 6),
    ((X, Y, Z), 0, 5),
    ((Y, X, Z), 1, 2),
    ((Z, Y, X), 0, 6),
    ((Z, X, Y), 1, 8),
)
SCALE_ORDER = (Y, Z, X)
ROWS = 16
ITEMS = {
    (4, 2, 2): (
        (0, 0), (0, 1), (4, 1), (0, 4), (4, 0), (0, 5), (4, 5), (2, 2), (2, 6), (0, 6),
        (2, 3), (4, 4), (3, 3), (1, 2), (3, 2), (1, 0), (6, 6), (2, 0), (5, 0), (1, 5),
        (5, 5), (7, 3), (1, 3), (2, 1), (0, 2), (1, 1), (5, 1), (2, 4), (6, 0), (1, 4),
        (5, 2), (6, 3), (4, 3), (3, 0), (7, 6), (6, 4), (3, 6), (4, 6), (5, 3), (3, 1),
        (4, 2), (6, 1), (2, 5), (7, 0), (7, 2), (6, 2), (3, 4), (5, 6), (6, 5), (1, 6),
        (3, 5), (7, 4), (5, 4), (0, 3), (7, 5), (7, 1),
    ),
}
WORD = 4
ONE_STAGE = 32


def grid_of(mesh):
    count = mesh.shape["shard"]
    at = [d.coords for d in mesh.devices.reshape(mesh.shape["pair"], count)[0]]
    sizes = tuple(len({c[d] for c in at}) for d in (2, 1, 0))
    return sizes


def power(base, exponent):
    result = jnp.float32(1.0)
    for bit in range(31):
        factor = jnp.float32(base ** (2**bit))
        result = jnp.where((exponent >> bit) & 1 == 1, result * factor, result)
    return result


def kernel(
    grid, limit_ref, step_ref, master_hbm, gradient_hbm, first_hbm, second_hbm,
    new_master, new_first, new_second, codes, scales,
    master, gradient, first, second, mine, my_scales, wide_scales, their_scales,
    group_sums, line_sums,
    load_sem, sum_send, group_recv, line_recv, send_sem, peer_scale_recv, recv_sem, local_sem,
):
    sizes = grid
    depth, high, wide = sizes
    plane = high * wide
    half_depth = depth // 2
    sources = half_depth * plane
    height, width = mine.shape
    tiles = width // LANES
    pieces = len(PIECES)
    core = lax.axis_index("pair")
    chip = lax.axis_index("shard")
    here = (chip // plane, (chip // wide) % high, chip % wide)
    keeper = here[Z] // half_depth
    peer = 1 - core

    def chip_at(at):
        return (at[Z] * high + at[Y]) * wide + at[X]

    def wait_bytes(ref, sem):
        pltpu.make_async_copy(ref, ref, sem).wait()

    loads = [
        pltpu.make_async_copy(source, held, load_sem.at[i])
        for i, (source, held) in enumerate(
            ((gradient_hbm, gradient), (master_hbm, master), (first_hbm, first), (second_hbm, second))
        )
    ]
    loads[0].start()
    barrier = pltpu.get_barrier_semaphore()
    chips = depth * plane
    one_stage = 2 * chips <= ONE_STAGE
    if one_stage:
        group = 2 * chips
        my_place = core * chips + chip
    else:
        group = 2 * plane
        my_place = core * plane + here[Y] * wide + here[X]

    def member(place):
        if one_stage:
            return (place // chips, place % chips)
        return (place // plane, here[Z] * plane + place % plane)

    def greet(device):
        pl.semaphore_signal(barrier, inc=1, device_id=device, device_id_type=MESH)

    def greet_member(place, carry):
        @pl.when(place != my_place)
        def _():
            greet(member(place))

        return carry

    lax.fori_loop(0, group, greet_member, 0)
    greeted = group - 1
    if not one_stage:
        for other in range(depth):
            @pl.when(other != here[Z])
            def _():
                for side in range(2):
                    greet((side, chip_at((other, here[Y], here[X]))))

        greeted += 2 * (depth - 1)

    for load in loads[1:]:
        load.start()
    loads[0].wait()

    def square(i, totals):
        rows = gradient[pl.ds(pl.multiple_of(i * 8, 8), 8), :]
        totals = list(totals)
        for j in range(tiles):
            part = rows[:, j * LANES : (j + 1) * LANES]
            totals[j % 4] = totals[j % 4] + part * part
        return tuple(totals)

    totals = lax.fori_loop(
        0, height // 8, square, tuple(jnp.zeros((8, LANES), jnp.float32) for _ in range(4))
    )
    total = (totals[0] + totals[1]) + (totals[2] + totals[3])
    total = jnp.sum(jnp.sum(total, axis=0, keepdims=True), axis=1, keepdims=True)
    total = jnp.broadcast_to(total, (1, LANES))

    one = jnp.ones((1, 1), jnp.float32)
    first_gain = one / (one - power(beta_first, step_ref[0]))
    second_gain = one / (one - power(beta_second, step_ref[0]))
    step_gain = jnp.broadcast_to(learn_rate * first_gain, (1, LANES))
    second_gain = jnp.broadcast_to(second_gain, (1, LANES))
    norm_limit = jnp.full((1, LANES), limit_ref[0], jnp.float32)
    wide_scales[...] = jnp.zeros_like(wide_scales)

    pl.semaphore_wait(barrier, greeted)

    def exchange(value, buffer, place, count, device_of, recv):
        buffer[place] = value

        def copy(other):
            return pltpu.make_async_remote_copy(
                src_ref=buffer.at[place], dst_ref=buffer.at[place],
                send_sem=sum_send, recv_sem=recv,
                device_id=device_of(other), device_id_type=MESH,
            )

        def send(other, carry):
            @pl.when(other != place)
            def _():
                copy(other).start()

            return carry

        lax.fori_loop(0, count, send, 0)
        others = buffer.at[pl.ds(0, count - 1)]
        wait_bytes(others, recv)
        return jnp.sum(buffer[pl.ds(0, count)], axis=0)

    total = exchange(total, group_sums, my_place, group, member, group_recv)
    if not one_stage:
        total = exchange(
            total, line_sums, here[Z], depth,
            lambda other: (core, chip_at((other, here[Y], here[X]))), line_recv,
        )
    clip_factor = norm_limit / jnp.maximum(jnp.sqrt(total), norm_limit)
    clip_first = (1.0 - beta_first) * clip_factor
    clip_second = (1.0 - beta_second) * clip_factor * clip_factor
    for load in loads[1:]:
        load.wait()

    def children(source, order):
        last = jnp.int32(-1)
        for i, dim in enumerate(order):
            last = jnp.where(here[dim] != source[dim], i, last)
        ways = []
        for i, dim in enumerate(order):
            if sizes[dim] == 2:
                there = list(here)
                there[dim] = 1 - here[dim]
                ways.append((last < i, chip_at(there)))
            elif sizes[dim] > 2:
                for step in (1, -1):
                    there = list(here)
                    there[dim] = here[dim] + step
                    inside = (there[dim] >= 0) & (there[dim] < sizes[dim])
                    away = (here[dim] - source[dim]) * step > 0
                    ways.append((inside & ((last < i) | ((last == i) & away)), chip_at(there)))
        return ways

    spans = []
    at = [0, 0]
    for _, column, share in PIECES:
        spans.append((at[column], tiles * share // 16))
        at[column] += spans[-1][1]
    assert at == [tiles, tiles]

    def code_part(source, column, start, size):
        row = (chip_at(source) % sources) * height
        lane = column * width + start * LANES
        return codes.at[pl.ds(pl.multiple_of(row, ROWS), height), pl.ds(lane, size * LANES)]

    def code_slice(source, k):
        return code_part(source, PIECES[k][1], *spans[k])

    def scale_slice(source):
        row = (chip_at(source) % sources) * height
        return scales.at[pl.ds(pl.multiple_of(row, 16), height), :]

    strips = height // ROWS
    broad = 1
    while 2 * broad <= 2 * tiles:
        broad *= 2

    def blocks(count):
        if count <= broad:
            return codes.at[pl.ds(0, ROWS), pl.ds(0, count * LANES)]
        return codes.at[pl.ds(0, count // broad * ROWS), pl.ds(0, broad * LANES)]

    my_index = chip % sources

    def own_copy(column, k, start, size, to):
        return pltpu.make_async_remote_copy(
            src_ref=mine.at[:, pl.ds(start * LANES, size * LANES)],
            dst_ref=code_part(here, column, start, size),
            send_sem=send_sem, recv_sem=recv_sem.at[my_index, k],
            device_id=(keeper, to), device_id_type=MESH,
        )

    lane = lax.broadcasted_iota(jnp.int32, (1, LANES), 1)
    spread_row = lax.broadcasted_iota(jnp.int32, (LANES, LANES), 0)
    spread_column = lax.broadcasted_iota(jnp.int32, (LANES, LANES), 1)
    spread = (spread_row == spread_column // BLOCK * BLOCK).astype(jnp.float32).astype(jnp.bfloat16)
    per_tile = LANES // BLOCK
    assert tiles <= BLOCK

    def tile(j):
        where = (slice(None), pl.ds(pl.multiple_of(j * LANES, LANES), LANES))
        weight = master[where]
        slope = gradient[where]
        moment = beta_first * first[where] + clip_first * slope
        power_moment = beta_second * second[where] + clip_second * (slope * slope)
        new_first[where] = moment
        new_second[where] = power_moment
        scaled = power_moment * second_gain
        root = scaled * lax.rsqrt(scaled)
        weight = (1.0 - learn_rate * decay_rate) * weight - step_gain * moment / (root + adam_eps)
        new_master[where] = weight
        largest = jnp.abs(weight)
        shift = BLOCK // 2
        while shift:
            largest = jnp.maximum(largest, pltpu.roll(largest, LANES - shift, axis=1))
            shift //= 2
        scale = jnp.maximum(largest, scale_floor).astype(jnp.bfloat16)
        scale = jnp.dot(scale, spread, preferred_element_type=jnp.float32)
        mine[where] = (weight / scale).astype(jnp.bfloat16)
        wide_scales[...] = jnp.where(lane % BLOCK == j, scale, wide_scales[...])

    parts = ([], [])
    for k, (_, column, _) in enumerate(PIECES):
        start, size = spans[k]
        cuts = [0, size]
        if start == 0:
            cuts = [0, 1, 3, size] if size > 3 else [0, 1, size]
        parts[column].extend((k, start + a, b - a) for a, b in zip(cuts, cuts[1:]))
    my_ways = {order: children(here, order) for order, _, _ in PIECES}

    def one_tile(j, carry):
        tile(j)
        return carry

    def send_part(p, carry):
        begin, end = jnp.int32(0), jnp.int32(0)
        for c in range(2):
            for i, (_, first_tile, count) in enumerate(parts[c]):
                at = (core == c) & (p == i)
                begin = jnp.where(at, first_tile, begin)
                end = jnp.where(at, first_tile + count, end)
        lax.fori_loop(begin, end, one_tile, 0)

        for c in range(2):
            for i, (k, first_tile, count) in enumerate(parts[c]):
                @pl.when((core == c) & (p == i))
                def _():
                    for used, to in my_ways[PIECES[k][0]]:
                        @pl.when(used)
                        def _():
                            own_copy(c, k, first_tile, count, to).start()

                    @pl.when(c != keeper)
                    def _():
                        own_copy(c, k, first_tile, count, chip).start()

        return carry

    lax.fori_loop(0, max(len(p) for p in parts), send_part, 0)
    sent = jnp.int32(0)
    for k, (order, column, _) in enumerate(PIECES):
        amount = spans[k][1] * strips
        for used, _ in my_ways[order]:
            sent = sent + jnp.where((core == column) & used, amount, 0)
        sent = sent + jnp.where((core == column) & (column != keeper), amount, 0)

    place_row = spread_row % BLOCK
    target = (core * tiles + place_row) * per_tile + spread_row // BLOCK
    pick = ((place_row < tiles) & (spread_column == target)).astype(jnp.float32)
    placed = jnp.dot(
        wide_scales[...].astype(jnp.bfloat16), pick.astype(jnp.bfloat16),
        preferred_element_type=jnp.float32,
    )
    my_scales[...] = placed.astype(jnp.bfloat16)
    peer_scales = pltpu.make_async_remote_copy(
        src_ref=my_scales, dst_ref=their_scales, send_sem=send_sem,
        recv_sem=peer_scale_recv, device_id=(peer, chip), device_id_type=MESH,
    )

    def scale_copy(source, to):
        return pltpu.make_async_remote_copy(
            src_ref=scale_slice(source), dst_ref=scale_slice(source),
            send_sem=send_sem, recv_sem=recv_sem.at[chip_at(source) % sources, pieces],
            device_id=(core, to), device_id_type=MESH,
        )

    @pl.when(core != keeper)
    def _():
        peer_scales.start()

    @pl.when(core == keeper)
    def _():
        peer_scales.wait_recv()
        merged = my_scales[...] + their_scales[...]
        row = pl.ds(pl.multiple_of(my_index * height, 16), height)
        scales[row, :] = merged
        for used, to in children(here, SCALE_ORDER):
            @pl.when(used)
            def _():
                scale_copy(here, to).start()

    sent = sent + jnp.where(core != keeper, strips, 0)
    for used, _ in children(here, SCALE_ORDER):
        sent = sent + jnp.where((core == keeper) & used, strips, 0)

    @pl.when(core == keeper)
    def _():
        row = my_index * height
        own = codes.at[
            pl.ds(pl.multiple_of(row, ROWS), height),
            pl.ds(pl.multiple_of(core * width, LANES), width),
        ]
        pltpu.make_async_copy(mine, own, local_sem).start()

    low = core * half_depth
    top = low + half_depth - 1

    def source_of(q):
        i, j = q // plane, q % plane
        inside = low + (here[Z] - low + i + depth) % half_depth
        z = jnp.where(here[Z] >= top, top - i, jnp.where(here[Z] <= low, low + i, inside))
        return (z, (here[Y] + j // wide) % high, (here[X] + j % wide) % wide)

    def code_copy(source, k, to):
        part = code_slice(source, k)
        return pltpu.make_async_remote_copy(
            src_ref=part, dst_ref=part, send_sem=send_sem,
            recv_sem=recv_sem.at[chip_at(source) % sources, k],
            device_id=(core, to), device_id_type=MESH,
        )

    items = ITEMS.get(sizes)
    words = []
    if items:
        assert sorted(items) == [(q, k) for q in range(sources) for k in range(pieces + 1)]
        for start in range(0, len(items), WORD):
            chunk = items[start : start + WORD]
            words.append(sum((16 * q + k) << (7 * i) for i, (q, k) in enumerate(chunk)))

    def item_of(t):
        if not words:
            return t // (pieces + 1), t % (pieces + 1)
        word = jnp.int32(0)
        for i, held in enumerate(words):
            word = jnp.where(t // WORD == i, held, word)
        item = (word >> (7 * (t % WORD))) % 128
        return item // 16, item % 16

    def forward(t, carry):
        q, which = item_of(t)
        source = source_of(q)
        index = chip_at(source) % sources
        mine_too = chip_at(source) == chip

        for k, (order, column, _) in enumerate(PIECES):
            @pl.when((which == k) & jnp.logical_not(mine_too & (core == column)))
            def _():
                wait_bytes(code_slice(source, k), recv_sem.at[index, k])

            @pl.when((which == k) & jnp.logical_not(mine_too))
            def _():
                for used, to in children(source, order):
                    @pl.when(used)
                    def _():
                        code_copy(source, k, to).start()

        @pl.when((which == pieces) & jnp.logical_not(mine_too))
        def _():
            wait_bytes(scale_slice(source), recv_sem.at[index, pieces])
            for used, to in children(source, SCALE_ORDER):
                @pl.when(used)
                def _():
                    scale_copy(source, to).start()

        return carry

    def passed(q, sent):
        source = source_of(q)
        others = chip_at(source) != chip
        orders = [(order, spans[k][1] * strips) for k, (order, _, _) in enumerate(PIECES)]
        for order in sorted({order for order, _ in orders} | {SCALE_ORDER}):
            amount = sum(a for o, a in orders if o == order) + (order == SCALE_ORDER) * strips
            for used, _ in children(source, order):
                sent = sent + jnp.where(others & used, amount, 0)
        return sent

    sent = lax.fori_loop(0, sources, passed, sent)
    lax.fori_loop(0, sources * (pieces + 1), forward, 0)

    wait_bytes(group_sums.at[pl.ds(0, group - 1)], sum_send)
    if not one_stage:
        wait_bytes(line_sums.at[pl.ds(0, depth - 1)], sum_send)

    @pl.when(core == keeper)
    def _():
        wait_bytes(mine, local_sem)

    most = broad
    while 2 * most <= broad * (codes.shape[0] // ROWS):
        most *= 2

    def drain(i, carry):
        wait_bytes(blocks(most), send_sem)
        return carry

    lax.fori_loop(0, sent // most, drain, 0)
    part = most // 2
    while part:
        @pl.when((sent // part) % 2 == 1)
        def _():
            wait_bytes(blocks(part), send_sem)

        part //= 2


def per_device(grid, master, gradient, first_moment, second_moment, max_norm, step_count):
    height, width = master.shape
    plane = grid[1] * grid[2]
    sources = grid[0] * plane // 2
    pieces = len(PIECES)
    kept = sources * height
    state = jax.ShapeDtypeStruct(master.shape, jnp.float32)
    held = pltpu.VMEM(master.shape, jnp.float32)
    narrow = pltpu.VMEM((height, LANES), jnp.bfloat16)
    dma = pltpu.SemaphoreType.DMA
    vmem = pl.BlockSpec(memory_space=pltpu.VMEM)
    smem = pl.BlockSpec(memory_space=pltpu.SMEM)
    hbm = pl.BlockSpec(memory_space=pltpu.HBM)
    free = pl.BlockSpec(memory_space=pl.ANY)
    state_in = [
        pltpu.with_memory_space_constraint(a, pltpu.HBM)
        for a in (master, gradient, first_moment, second_moment)
    ]
    results = pl.pallas_call(
        functools.partial(kernel, grid),
        out_shape=(
            state, state, state,
            jax.ShapeDtypeStruct((kept, 2 * width), jnp.bfloat16),
            jax.ShapeDtypeStruct((kept, 2 * width // BLOCK), jnp.bfloat16),
        ),
        in_specs=[smem, smem, hbm, hbm, hbm, hbm],
        out_specs=(vmem, vmem, vmem, free, vmem),
        scratch_shapes=[
            held, held, held, held,
            pltpu.VMEM((height, width), jnp.bfloat16),
            narrow,
            pltpu.VMEM((height, LANES), jnp.float32),
            narrow,
            pltpu.VMEM((max(2 * plane, ONE_STAGE), 1, LANES), jnp.float32),
            pltpu.VMEM((grid[0], 1, LANES), jnp.float32),
            dma((4,)), dma(()), dma(()), dma(()), dma(()), dma(()),
            dma((sources, pieces + 1)), dma(()),
        ],
        compiler_params=pltpu.CompilerParams(
            collective_id=0, has_side_effects=True, vmem_limit_bytes=KERNEL_VMEM
        ),
    )(max_norm, step_count, *state_in)
    return pl.pallas_call(
        flush,
        out_shape=tuple(jax.ShapeDtypeStruct(r.shape, r.dtype) for r in results),
        in_specs=[free] * len(results),
        out_specs=(hbm,) * len(results),
        scratch_shapes=[dma((len(results), PARTS))],
        compiler_params=pltpu.CompilerParams(vmem_limit_bytes=FLUSH_VMEM),
    )(*results)


def flush(*refs):
    count = len(refs) // 2
    sem = refs[-1]
    copies = []
    for i, (held, out) in enumerate(zip(refs[:count], refs[count:-1])):
        rows = held.shape[0] // PARTS
        for part in range(PARTS):
            span = pl.ds(part * rows, rows)
            copies.append(pltpu.make_async_copy(held.at[span], out.at[span], sem.at[i, part]))
    for copy in copies:
        copy.start()
    for copy in copies:
        copy.wait()


PARTS = 2
FLUSH_VMEM = 1024 * 1024


KERNEL_VMEM = 16 * 1024 * 1024


def solution(mesh):
    return jax.shard_map(
        functools.partial(per_device, grid_of(mesh)),
        mesh=mesh,
        in_specs=(
            P("shard", "pair"),
            P("shard", "pair"),
            P("shard", "pair"),
            P("shard", "pair"),
            P(),
            P(),
        ),
        out_specs=(
            P("shard", "pair"),
            P("shard", "pair"),
            P("shard", "pair"),
            P("pair", None),
            P("pair", None),
        ),
        check_vma=False,
    )
```

```python
import functools

import jax
import jax.numpy as jnp
from jax import lax
from jax.experimental import pallas as pl
from jax.experimental.pallas import tpu as pltpu
from jax.sharding import PartitionSpec as P

BLOCK = 32
LANES = 128

beta_first = 0.9
beta_second = 0.99
learn_rate = 0.01
decay_rate = 0.1
adam_eps = 1e-06
scale_floor = 0.25

MESH = pl.DeviceIdType.MESH
Z, Y, X = 0, 1, 2
PIECES = (
    ((Z, X, Y), 0, 5),
    ((Z, Y, X), 1, 6),
    ((X, Y, Z), 0, 5),
    ((Y, X, Z), 1, 2),
    ((Z, Y, X), 0, 6),
    ((Z, X, Y), 1, 8),
)
SCALE_ORDER = (Y, Z, X)
ROWS = 16
ITEMS = {
    (4, 2, 2): (
        (0, 0), (0, 1), (4, 1), (0, 4), (4, 0), (0, 5), (4, 5), (2, 2), (2, 6), (0, 6),
        (2, 3), (4, 4), (3, 3), (1, 2), (3, 2), (1, 0), (6, 6), (2, 0), (5, 0), (1, 5),
        (5, 5), (7, 3), (1, 3), (2, 1), (0, 2), (1, 1), (5, 1), (2, 4), (6, 0), (1, 4),
        (5, 2), (6, 3), (4, 3), (3, 0), (7, 6), (6, 4), (3, 6), (4, 6), (5, 3), (3, 1),
        (4, 2), (6, 1), (2, 5), (7, 0), (7, 2), (6, 2), (3, 4), (5, 6), (6, 5), (1, 6),
        (3, 5), (7, 4), (5, 4), (0, 3), (7, 5), (7, 1),
    ),
}
WORD = 4
ONE_STAGE = 32


def grid_of(mesh):
    count = mesh.shape["shard"]
    at = [d.coords for d in mesh.devices.reshape(mesh.shape["pair"], count)[0]]
    sizes = tuple(len({c[d] for c in at}) for d in (2, 1, 0))
    return sizes


def power(base, exponent):
    result = jnp.float32(1.0)
    for bit in range(31):
        factor = jnp.float32(base ** (2**bit))
        result = jnp.where((exponent >> bit) & 1 == 1, result * factor, result)
    return result


def kernel(
    grid, limit_ref, step_ref, master_hbm, gradient_hbm, first_hbm, second_hbm,
    new_master, new_first, new_second, codes, scales,
    master, gradient, first, second, mine, my_scales, wide_scales, their_scales,
    group_sums, line_sums,
    load_sem, sum_send, group_recv, line_recv, send_sem, peer_scale_recv, recv_sem, local_sem,
):
    sizes = grid
    depth, high, wide = sizes
    plane = high * wide
    half_depth = depth // 2
    sources = half_depth * plane
    height, width = mine.shape
    tiles = width // LANES
    pieces = len(PIECES)
    core = lax.axis_index("pair")
    chip = lax.axis_index("shard")
    here = (chip // plane, (chip // wide) % high, chip % wide)
    keeper = here[Z] // half_depth
    peer = 1 - core

    def chip_at(at):
        return (at[Z] * high + at[Y]) * wide + at[X]

    def wait_bytes(ref, sem):
        pltpu.make_async_copy(ref, ref, sem).wait()

    loads = [
        pltpu.make_async_copy(source, held, load_sem.at[i])
        for i, (source, held) in enumerate(
            ((gradient_hbm, gradient), (master_hbm, master), (first_hbm, first), (second_hbm, second))
        )
    ]
    loads[0].start()
    barrier = pltpu.get_barrier_semaphore()
    chips = depth * plane
    one_stage = 2 * chips <= ONE_STAGE
    if one_stage:
        group = 2 * chips
        my_place = core * chips + chip
    else:
        group = 2 * plane
        my_place = core * plane + here[Y] * wide + here[X]

    def member(place):
        if one_stage:
            return (place // chips, place % chips)
        return (place // plane, here[Z] * plane + place % plane)

    def greet(device):
        pl.semaphore_signal(barrier, inc=1, device_id=device, device_id_type=MESH)

    def greet_member(place, carry):
        @pl.when(place != my_place)
        def _():
            greet(member(place))

        return carry

    lax.fori_loop(0, group, greet_member, 0)
    greeted = group - 1
    if not one_stage:
        for other in range(depth):
            @pl.when(other != here[Z])
            def _():
                for side in range(2):
                    greet((side, chip_at((other, here[Y], here[X]))))

        greeted += 2 * (depth - 1)

    for load in loads[1:]:
        load.start()
    loads[0].wait()

    def square(i, totals):
        rows = gradient[pl.ds(pl.multiple_of(i * 8, 8), 8), :]
        totals = list(totals)
        for j in range(tiles):
            part = rows[:, j * LANES : (j + 1) * LANES]
            totals[j % 4] = totals[j % 4] + part * part
        return tuple(totals)

    totals = lax.fori_loop(
        0, height // 8, square, tuple(jnp.zeros((8, LANES), jnp.float32) for _ in range(4))
    )
    total = (totals[0] + totals[1]) + (totals[2] + totals[3])
    total = jnp.sum(jnp.sum(total, axis=0, keepdims=True), axis=1, keepdims=True)
    total = jnp.broadcast_to(total, (1, LANES))

    one = jnp.ones((1, 1), jnp.float32)
    first_gain = one / (one - power(beta_first, step_ref[0]))
    second_gain = one / (one - power(beta_second, step_ref[0]))
    step_gain = jnp.broadcast_to(learn_rate * first_gain, (1, LANES))
    second_gain = jnp.broadcast_to(second_gain, (1, LANES))
    norm_limit = jnp.full((1, LANES), limit_ref[0], jnp.float32)
    wide_scales[...] = jnp.zeros_like(wide_scales)

    pl.semaphore_wait(barrier, greeted)

    def exchange(value, buffer, place, count, device_of, recv):
        buffer[place] = value

        def copy(other):
            return pltpu.make_async_remote_copy(
                src_ref=buffer.at[place], dst_ref=buffer.at[place],
                send_sem=sum_send, recv_sem=recv,
                device_id=device_of(other), device_id_type=MESH,
            )

        def send(other, carry):
            @pl.when(other != place)
            def _():
                copy(other).start()

            return carry

        lax.fori_loop(0, count, send, 0)
        others = buffer.at[pl.ds(0, count - 1)]
        wait_bytes(others, recv)
        return jnp.sum(buffer[pl.ds(0, count)], axis=0)

    total = exchange(total, group_sums, my_place, group, member, group_recv)
    if not one_stage:
        total = exchange(
            total, line_sums, here[Z], depth,
            lambda other: (core, chip_at((other, here[Y], here[X]))), line_recv,
        )
    clip_factor = norm_limit / jnp.maximum(jnp.sqrt(total), norm_limit)
    clip_first = (1.0 - beta_first) * clip_factor
    clip_second = (1.0 - beta_second) * clip_factor * clip_factor
    for load in loads[1:]:
        load.wait()

    def children(source, order):
        last = jnp.int32(-1)
        for i, dim in enumerate(order):
            last = jnp.where(here[dim] != source[dim], i, last)
        ways = []
        for i, dim in enumerate(order):
            if sizes[dim] == 2:
                there = list(here)
                there[dim] = 1 - here[dim]
                ways.append((last < i, chip_at(there)))
            elif sizes[dim] > 2:
                for step in (1, -1):
                    there = list(here)
                    there[dim] = here[dim] + step
                    inside = (there[dim] >= 0) & (there[dim] < sizes[dim])
                    away = (here[dim] - source[dim]) * step > 0
                    ways.append((inside & ((last < i) | ((last == i) & away)), chip_at(there)))
        return ways

    spans = []
    at = [0, 0]
    for _, column, share in PIECES:
        spans.append((at[column], tiles * share // 16))
        at[column] += spans[-1][1]
    assert at == [tiles, tiles]

    def code_part(source, column, start, size):
        row = (chip_at(source) % sources) * height
        lane = column * width + start * LANES
        return codes.at[pl.ds(pl.multiple_of(row, ROWS), height), pl.ds(lane, size * LANES)]

    def code_slice(source, k):
        return code_part(source, PIECES[k][1], *spans[k])

    def scale_slice(source):
        row = (chip_at(source) % sources) * height
        return scales.at[pl.ds(pl.multiple_of(row, 16), height), :]

    strips = height // ROWS
    broad = 1
    while 2 * broad <= 2 * tiles:
        broad *= 2

    def blocks(count):
        if count <= broad:
            return codes.at[pl.ds(0, ROWS), pl.ds(0, count * LANES)]
        return codes.at[pl.ds(0, count // broad * ROWS), pl.ds(0, broad * LANES)]

    my_index = chip % sources

    def own_copy(column, k, start, size, to):
        return pltpu.make_async_remote_copy(
            src_ref=mine.at[:, pl.ds(start * LANES, size * LANES)],
            dst_ref=code_part(here, column, start, size),
            send_sem=send_sem, recv_sem=recv_sem.at[my_index, k],
            device_id=(keeper, to), device_id_type=MESH,
        )

    lane = lax.broadcasted_iota(jnp.int32, (1, LANES), 1)
    spread_row = lax.broadcasted_iota(jnp.int32, (LANES, LANES), 0)
    spread_column = lax.broadcasted_iota(jnp.int32, (LANES, LANES), 1)
    per_tile = LANES // BLOCK
    assert tiles <= BLOCK

    def tile(j):
        where = (slice(None), pl.ds(pl.multiple_of(j * LANES, LANES), LANES))
        weight = master[where]
        slope = gradient[where]
        moment = beta_first * first[where] + clip_first * slope
        power_moment = beta_second * second[where] + clip_second * (slope * slope)
        new_first[where] = moment
        new_second[where] = power_moment
        scaled = power_moment * second_gain
        root = scaled * lax.rsqrt(scaled)
        weight = (1.0 - learn_rate * decay_rate) * weight - step_gain * moment / (root + adam_eps)
        new_master[where] = weight
        largest = jnp.abs(weight)
        shift = BLOCK // 2
        while shift:
            ahead = pltpu.roll(largest, LANES - shift, axis=1)
            behind = pltpu.roll(largest, shift, axis=1)
            largest = jnp.maximum(largest, jnp.where((lane & shift) == 0, ahead, behind))
            shift //= 2
        scale = jnp.maximum(largest, scale_floor).astype(jnp.bfloat16)
        scale = scale.astype(jnp.float32)
        mine[where] = (weight / scale).astype(jnp.bfloat16)
        wide_scales[...] = jnp.where(lane % BLOCK == j, scale, wide_scales[...])

    parts = ([], [])
    for k, (_, column, _) in enumerate(PIECES):
        start, size = spans[k]
        cuts = [0, size]
        if start == 0:
            cuts = [0, 1, 3, size] if size > 3 else [0, 1, size]
        parts[column].extend((k, start + a, b - a) for a, b in zip(cuts, cuts[1:]))
    my_ways = {order: children(here, order) for order, _, _ in PIECES}

    def one_tile(j, carry):
        tile(j)
        return carry

    def send_part(p, carry):
        begin, end = jnp.int32(0), jnp.int32(0)
        for c in range(2):
            for i, (_, first_tile, count) in enumerate(parts[c]):
                at = (core == c) & (p == i)
                begin = jnp.where(at, first_tile, begin)
                end = jnp.where(at, first_tile + count, end)
        lax.fori_loop(begin, end, one_tile, 0)

        for c in range(2):
            for i, (k, first_tile, count) in enumerate(parts[c]):
                @pl.when((core == c) & (p == i))
                def _():
                    for used, to in my_ways[PIECES[k][0]]:
                        @pl.when(used)
                        def _():
                            own_copy(c, k, first_tile, count, to).start()

                    @pl.when(c != keeper)
                    def _():
                        own_copy(c, k, first_tile, count, chip).start()

        return carry

    lax.fori_loop(0, max(len(p) for p in parts), send_part, 0)
    sent = jnp.int32(0)
    for k, (order, column, _) in enumerate(PIECES):
        amount = spans[k][1] * strips
        for used, _ in my_ways[order]:
            sent = sent + jnp.where((core == column) & used, amount, 0)
        sent = sent + jnp.where((core == column) & (column != keeper), amount, 0)

    place_row = spread_row % BLOCK
    target = (core * tiles + place_row) * per_tile + spread_row // BLOCK
    pick = ((place_row < tiles) & (spread_column == target)).astype(jnp.float32)
    placed = jnp.dot(
        wide_scales[...].astype(jnp.bfloat16), pick.astype(jnp.bfloat16),
        preferred_element_type=jnp.float32,
    )
    my_scales[...] = placed.astype(jnp.bfloat16)
    peer_scales = pltpu.make_async_remote_copy(
        src_ref=my_scales, dst_ref=their_scales, send_sem=send_sem,
        recv_sem=peer_scale_recv, device_id=(peer, chip), device_id_type=MESH,
    )

    def scale_copy(source, to):
        return pltpu.make_async_remote_copy(
            src_ref=scale_slice(source), dst_ref=scale_slice(source),
            send_sem=send_sem, recv_sem=recv_sem.at[chip_at(source) % sources, pieces],
            device_id=(core, to), device_id_type=MESH,
        )

    @pl.when(core != keeper)
    def _():
        peer_scales.start()

    @pl.when(core == keeper)
    def _():
        peer_scales.wait_recv()
        merged = my_scales[...] + their_scales[...]
        row = pl.ds(pl.multiple_of(my_index * height, 16), height)
        scales[row, :] = merged
        for used, to in children(here, SCALE_ORDER):
            @pl.when(used)
            def _():
                scale_copy(here, to).start()

    sent = sent + jnp.where(core != keeper, strips, 0)
    for used, _ in children(here, SCALE_ORDER):
        sent = sent + jnp.where((core == keeper) & used, strips, 0)

    @pl.when(core == keeper)
    def _():
        row = my_index * height
        own = codes.at[
            pl.ds(pl.multiple_of(row, ROWS), height),
            pl.ds(pl.multiple_of(core * width, LANES), width),
        ]
        pltpu.make_async_copy(mine, own, local_sem).start()

    low = core * half_depth
    top = low + half_depth - 1

    def source_of(q):
        i, j = q // plane, q % plane
        inside = low + (here[Z] - low + i + depth) % half_depth
        z = jnp.where(here[Z] >= top, top - i, jnp.where(here[Z] <= low, low + i, inside))
        return (z, (here[Y] + j // wide) % high, (here[X] + j % wide) % wide)

    def code_copy(source, k, to):
        part = code_slice(source, k)
        return pltpu.make_async_remote_copy(
            src_ref=part, dst_ref=part, send_sem=send_sem,
            recv_sem=recv_sem.at[chip_at(source) % sources, k],
            device_id=(core, to), device_id_type=MESH,
        )

    items = ITEMS.get(sizes)
    words = []
    if items:
        assert sorted(items) == [(q, k) for q in range(sources) for k in range(pieces + 1)]
        for start in range(0, len(items), WORD):
            chunk = items[start : start + WORD]
            words.append(sum((16 * q + k) << (7 * i) for i, (q, k) in enumerate(chunk)))

    def item_of(t):
        if not words:
            return t // (pieces + 1), t % (pieces + 1)
        word = jnp.int32(0)
        for i, held in enumerate(words):
            word = jnp.where(t // WORD == i, held, word)
        item = (word >> (7 * (t % WORD))) % 128
        return item // 16, item % 16

    def forward(t, carry):
        q, which = item_of(t)
        source = source_of(q)
        index = chip_at(source) % sources
        mine_too = chip_at(source) == chip

        for k, (order, column, _) in enumerate(PIECES):
            @pl.when((which == k) & jnp.logical_not(mine_too & (core == column)))
            def _():
                wait_bytes(code_slice(source, k), recv_sem.at[index, k])

            @pl.when((which == k) & jnp.logical_not(mine_too))
            def _():
                for used, to in children(source, order):
                    @pl.when(used)
                    def _():
                        code_copy(source, k, to).start()

        @pl.when((which == pieces) & jnp.logical_not(mine_too))
        def _():
            wait_bytes(scale_slice(source), recv_sem.at[index, pieces])
            for used, to in children(source, SCALE_ORDER):
                @pl.when(used)
                def _():
                    scale_copy(source, to).start()

        return carry

    def passed(q, sent):
        source = source_of(q)
        others = chip_at(source) != chip
        orders = [(order, spans[k][1] * strips) for k, (order, _, _) in enumerate(PIECES)]
        for order in sorted({order for order, _ in orders} | {SCALE_ORDER}):
            amount = sum(a for o, a in orders if o == order) + (order == SCALE_ORDER) * strips
            for used, _ in children(source, order):
                sent = sent + jnp.where(others & used, amount, 0)
        return sent

    sent = lax.fori_loop(0, sources, passed, sent)
    lax.fori_loop(0, sources * (pieces + 1), forward, 0)

    wait_bytes(group_sums.at[pl.ds(0, group - 1)], sum_send)
    if not one_stage:
        wait_bytes(line_sums.at[pl.ds(0, depth - 1)], sum_send)

    @pl.when(core == keeper)
    def _():
        wait_bytes(mine, local_sem)

    most = broad
    while 2 * most <= broad * (codes.shape[0] // ROWS):
        most *= 2

    def drain(i, carry):
        wait_bytes(blocks(most), send_sem)
        return carry

    lax.fori_loop(0, sent // most, drain, 0)
    part = most // 2
    while part:
        @pl.when((sent // part) % 2 == 1)
        def _():
            wait_bytes(blocks(part), send_sem)

        part //= 2


def per_device(grid, master, gradient, first_moment, second_moment, max_norm, step_count):
    height, width = master.shape
    plane = grid[1] * grid[2]
    sources = grid[0] * plane // 2
    pieces = len(PIECES)
    kept = sources * height
    state = jax.ShapeDtypeStruct(master.shape, jnp.float32)
    held = pltpu.VMEM(master.shape, jnp.float32)
    narrow = pltpu.VMEM((height, LANES), jnp.bfloat16)
    dma = pltpu.SemaphoreType.DMA
    vmem = pl.BlockSpec(memory_space=pltpu.VMEM)
    smem = pl.BlockSpec(memory_space=pltpu.SMEM)
    hbm = pl.BlockSpec(memory_space=pltpu.HBM)
    free = pl.BlockSpec(memory_space=pl.ANY)
    state_in = [
        pltpu.with_memory_space_constraint(a, pltpu.HBM)
        for a in (master, gradient, first_moment, second_moment)
    ]
    results = pl.pallas_call(
        functools.partial(kernel, grid),
        out_shape=(
            state, state, state,
            jax.ShapeDtypeStruct((kept, 2 * width), jnp.bfloat16),
            jax.ShapeDtypeStruct((kept, 2 * width // BLOCK), jnp.bfloat16),
        ),
        in_specs=[smem, smem, hbm, hbm, hbm, hbm],
        out_specs=(vmem, vmem, vmem, free, vmem),
        scratch_shapes=[
            held, held, held, held,
            pltpu.VMEM((height, width), jnp.bfloat16),
            narrow,
            pltpu.VMEM((height, LANES), jnp.float32),
            narrow,
            pltpu.VMEM((max(2 * plane, ONE_STAGE), 1, LANES), jnp.float32),
            pltpu.VMEM((grid[0], 1, LANES), jnp.float32),
            dma((4,)), dma(()), dma(()), dma(()), dma(()), dma(()),
            dma((sources, pieces + 1)), dma(()),
        ],
        compiler_params=pltpu.CompilerParams(
            collective_id=0, has_side_effects=True, vmem_limit_bytes=KERNEL_VMEM
        ),
    )(max_norm, step_count, *state_in)
    return pl.pallas_call(
        flush,
        out_shape=tuple(jax.ShapeDtypeStruct(r.shape, r.dtype) for r in results),
        in_specs=[free] * len(results),
        out_specs=(hbm,) * len(results),
        scratch_shapes=[dma((len(results), PARTS))],
        compiler_params=pltpu.CompilerParams(vmem_limit_bytes=FLUSH_VMEM),
    )(*results)


def flush(*refs):
    count = len(refs) // 2
    sem = refs[-1]
    copies = []
    for i, (held, out) in enumerate(zip(refs[:count], refs[count:-1])):
        rows = held.shape[0] // PARTS
        for part in range(PARTS):
            span = pl.ds(part * rows, rows)
            copies.append(pltpu.make_async_copy(held.at[span], out.at[span], sem.at[i, part]))
    for copy in copies:
        copy.start()
    for copy in copies:
        copy.wait()


PARTS = 2
FLUSH_VMEM = 1024 * 1024


KERNEL_VMEM = 16 * 1024 * 1024


def solution(mesh):
    return jax.shard_map(
        functools.partial(per_device, grid_of(mesh)),
        mesh=mesh,
        in_specs=(
            P("shard", "pair"),
            P("shard", "pair"),
            P("shard", "pair"),
            P("shard", "pair"),
            P(),
            P(),
        ),
        out_specs=(
            P("shard", "pair"),
            P("shard", "pair"),
            P("shard", "pair"),
            P("pair", None),
            P("pair", None),
        ),
        check_vma=False,
    )
```
